256 devices in a mesh: row: 8 (over x, core), col: 4 (over y), depth: 8 (over z).
Axes of the slice: x: 4, y: 4, z: 8, core: 2. Of those that a mesh axis runs over, the one named last changes fastest.
Arguments:
- left_values: bfloat16 [384, 32, 4, 529], P('row', ('col', 'depth')), may hold values from -1.25 to 1.25
- left_columns: int32 [384, 32, 4], P('row', ('col', 'depth')), may hold values from 0 to 39, as said below
- right_values: bfloat16 [32, 40, 4, 3, 529], P(('col', 'depth'), 'row'), may hold values from -1.75 to 1.75
- right_columns: int32 [32, 40, 4, 3], P(('col', 'depth'), 'row'), may hold values from 0 to 31, as said below
Outputs:
- product_matrix: bfloat16 [8832, 2944], P('row', ('col', 'depth'))
The draws below stay inside these ranges and needn't reach their ends.
Inputs may be any that keep to these rules, and one draw needn't show every extreme that they name: `left_columns`: within one block row and panel the 4 entries are distinct. `right_columns`: within one block row and column tile the 3 entries are distinct.
All inputs are finite; a program needn't handle non-finite values.
Results may differ from the reference program's by a relative error of at most 0.001.
Values may be sent and summed in bfloat16 or wider, within the bound.
A program may use at most 128 MiB of HBM per device.

```python
import jax
import jax.numpy as jnp
from jax import lax

BLK = 23
PANEL = 40
KPAN = 32
SAP = 4
CT = 4
CTW = 32
SBP = 3
MB = 384
NB = 128


def distinct_columns(key, leading, choices, count):
    scores = jax.random.randint(key, leading + (choices,), 0, 1 << 20) * choices + jnp.arange(choices, dtype=jnp.int32)
    chosen = lax.top_k(scores, count)[1]
    return chosen.astype(jnp.int32)


def draw_left_columns(key, part):
    return distinct_columns(jax.random.fold_in(key, 11), (MB, KPAN), PANEL, SAP)


def draw_right_columns(key, part):
    return distinct_columns(jax.random.fold_in(key, 12), (KPAN, PANEL, CT), CTW, SBP)


def level_of(own_key, shape, pieces, smallest, high):
    factor_of, own = 1.0, jax.random.fold_in(own_key, 6)
    for dim, blocks in pieces:
        draws = jnp.exp(jax.random.uniform(jax.random.fold_in(own, dim), (blocks,), jnp.float32, smallest / len(pieces), high / len(pieces)))
        factor_of = factor_of * jnp.repeat(draws, shape[dim] // blocks).reshape([-1 if axis == dim else 1 for axis in range(len(shape))])
    return factor_of


def centred(rng, shape, width, most, pieces=(), held_as=jnp.bfloat16):
    loudness = level_of(rng, shape, pieces, -0.22, 0.18) if pieces else 1.0
    result = jax.random.normal(rng, shape, jnp.float32) * width * loudness
    return jnp.minimum(jnp.maximum(result, -most), most).astype(held_as)


def setup_inputs(seed: int = 0) -> dict:
    key_list = jax.random.split(jax.random.key(seed), 5)
    return {
        "left_values": centred(key_list[0], (MB, KPAN, SAP, BLK * BLK), BLK ** -0.5, 1.25, ((0, 8), (1, 32))),
        "left_columns": draw_left_columns(jax.random.fold_in(key_list[4], 71), 0),
        "right_values": centred(key_list[2], (KPAN, PANEL, CT, SBP, BLK * BLK), (SAP * SBP * KPAN // CTW) ** -0.5, 1.75, ((0, 32), (1, 8))),
        "right_columns": draw_right_columns(jax.random.fold_in(key_list[4], 71), 0),
    }


def reference(left_values, left_columns, right_values, right_columns):
    tile_base = (jnp.arange(CT, dtype=jnp.int32) * CTW)[None, None, :, None]
    row_ids = jnp.broadcast_to(jnp.arange(MB, dtype=jnp.int32)[:, None], (MB, SAP * CT * SBP))

    def panel_step(running, items):
        left_panel, left_cols, right_panel, right_cols = items
        chosen = right_panel[left_cols]
        chosen_cols = right_cols[left_cols] + tile_base
        left_mats = left_panel.astype(jnp.float32).reshape(MB, SAP, BLK, BLK)
        right_mats = chosen.astype(jnp.float32).reshape(MB, SAP, CT * SBP, BLK, BLK)
        partial_blocks = jnp.einsum("isab,isnbc->isnac", left_mats, right_mats, precision=lax.Precision.HIGHEST)
        partial_blocks = partial_blocks.reshape(MB, SAP * CT * SBP, BLK * BLK)
        running = running.at[row_ids, chosen_cols.reshape(MB, SAP * CT * SBP)].add(partial_blocks)
        return running, None

    start_blocks = jnp.zeros((MB, NB, BLK * BLK), jnp.float32)
    items = (jnp.transpose(left_values, (1, 0, 2, 3)), jnp.transpose(left_columns, (1, 0, 2)), right_values, right_columns)
    summed, unused = lax.scan(panel_step, start_blocks, items)
    dense = jnp.transpose(summed.reshape(MB, NB, BLK, BLK), (0, 2, 1, 3)).reshape(MB * BLK, NB * BLK)
    return dense.astype(jnp.bfloat16)
```

```python
import jax
import jax.numpy as jnp
from jax import lax
from jax.experimental import pallas as pl
from jax.experimental.pallas import tpu as pltpu
from jax.sharding import PartitionSpec as P

MESH = pl.DeviceIdType.MESH
BF = jnp.bfloat16
F32 = jnp.float32
I32 = jnp.int32
SQ = 529


def iota(shape, dim):
    return lax.broadcasted_iota(I32, shape, dim)


def onehot(cond):
    return jnp.where(cond, 1.0, 0.0).astype(BF)


def div25(lane):
    return (lane * 41) >> 10


def div23(n):
    return (n * 2850) >> 16


def prepare(left_ref, right_ref, lw_ref, rw_ref):
    lane = iota((1, 128), 1)
    field = iota((SQ + 1, 128), 0)
    left = left_ref[...]
    tiles = []
    for t in range(5):
        target = jnp.where(lane < 115, 115 * t + lane, 9999)
        target = jnp.where(target < SQ, target, 9999)
        target = jnp.where(lane == 120, SQ, target)
        tiles.append(jnp.dot(left, onehot(field == target), preferred_element_type=F32))
    for d in range(8):
        rows = [tile[24 * d : 24 * d + 24] for tile in tiles] + [jnp.zeros((8, 128), F32)]
        lw_ref[d] = jnp.concatenate(rows, axis=0).astype(BF)
    right = right_ref[...]
    row = iota((288, 1), 0)
    group = (row * 2731) >> 16
    c = row - 24 * group
    f = iota((288, SQ + 1), 1)
    f_c = f - 23 * div23(f)
    keep = jnp.where(f == SQ, 23, f_c) == c
    q_of = div25(lane)
    b_of = lane - 25 * q_of
    total = jnp.zeros((288, 128), F32)
    for q in range(5):
        pick = onehot(iota((288, 60), 1) == group + 12 * q)
        spread = jnp.dot(pick, right, preferred_element_type=F32)
        spread = jnp.where(keep, spread, 0.0).astype(BF)
        low = jnp.where(q_of == q, 23 * b_of, 9999)
        hit = jnp.where((field >= low) & (field < low + 23) & (field < SQ), 1.0, 0.0)
        code = jnp.where((field == SQ) & (q_of == q), 1.0, 0.0)
        total += jnp.dot(spread, (hit + code).astype(BF), preferred_element_type=F32)
    for t in range(4):
        rw_ref[t] = total[72 * t : 72 * t + 72].astype(BF)


def multiply(
    lws, rws, out, LW, RW, PX, VE, LD, RT, ACC, OS,
    a_s, a_r, b_s, b_r, z_s, z_r, x_s, x_r, xh_s, xh_r, y_s, y_r, yh_s, yh_r, d_s, d_r, o_s, o_r, l_sem,
):
    r, y, z = lax.axis_index("row"), lax.axis_index("col"), lax.axis_index("depth")
    x, e = r // 2, r % 2
    mod = lax.rem

    def zat(o):
        return (r, y, mod(z + o + 8, 8))

    def yat(o):
        return (r, mod(y + o + 4, 4), z)

    def xat(o):
        return (mod(r + 2 * o + 8, 8), y, z)

    partner = (r + 1 - 2 * e, y, z)
    friends = [zat(o) for o in range(1, 8)] + [yat(o) for o in range(1, 4)] + [xat(1), xat(-1), partner]
    barrier = pltpu.get_barrier_semaphore()
    for who in friends:
        pl.semaphore_signal(barrier, inc=1, device_id=who, device_id_type=MESH)
    pl.semaphore_wait(barrier, len(friends))

    def copy(src, dst, send, recv, who):
        return pltpu.make_async_remote_copy(
            src_ref=src, dst_ref=dst, send_sem=send, recv_sem=recv, device_id=who, device_id_type=MESH
        )

    def unit(k):
        odd = k % 2
        return mod(z + (1 - 2 * odd) * ((k + 1) // 2) + 8, 8)

    def a_copy(o):
        to = mod(y + o, 4)
        return copy(rws.at[to], RW.at[z, e, x, y], a_s.at[o - 1], a_r.at[o - 1], (r, to, z))

    def b_copy(k):
        odd = k % 2
        to = mod(z - (1 - 2 * odd) * ((k + 1) // 2) + 8, 8)
        return copy(lws.at[to], LW.at[y, z], b_s.at[k], b_r.at[k], (r, y, to))

    def z_copy(k):
        odd = k % 2
        step = 2 * odd - 1
        u = mod(z - (2 * odd - 1) * ((k + 1) // 2 - 1) + 8, 8)
        ref = RW.at[u, e, x]
        return copy(ref, ref, z_s.at[k], z_r.at[k], (r, y, mod(z + step + 8, 8)))

    def zh_copy(h):
        u = unit(5 + h)
        ref = RW.at[u, e, x, pl.ds(2 * h, 2)]
        return copy(ref, ref, z_s.at[7 + h], z_r.at[7 + h], zat(1 - 2 * h))

    def x_copy(k, h):
        ref = RW.at[unit(k), e, x]
        return copy(ref, ref, x_s.at[h, k], x_r.at[h, k], xat(1 - 2 * h))

    def xh_copy(k, h):
        ref = RW.at[unit(k), e, mod(x - (1 - 2 * h) + 4, 4), pl.ds(2 * h, 2)]
        return copy(ref, ref, xh_s.at[h, k], xh_r.at[h, k], xat(1 - 2 * h))

    def y_copy(k, h):
        ref = LW.at[y, unit(k)]
        return copy(ref, ref, y_s.at[h, k], y_r.at[h, k], yat(1 - 2 * h))

    def yh_copy(k, h):
        ref = LW.at[mod(y - (1 - 2 * h) + 4, 4), unit(k), pl.ds(64 * h, 64)]
        return copy(ref, ref, yh_s.at[h, k], yh_r.at[h, k], yat(1 - 2 * h))

    def d_copy(k):
        ref = RW.at[unit(k), e]
        return copy(ref, ref, d_s.at[k], d_r.at[k], partner)

    for o in range(1, 4):
        a_copy(o).start()
    for k in range(1, 8):
        b_copy(k).start()
    own_right = pltpu.make_async_copy(rws.at[y], RW.at[z, e, x, y], l_sem.at[0])
    own_right.start()
    own_left = pltpu.make_async_copy(lws.at[z], LW.at[y, z], l_sem.at[1])
    own_left.start()

    lane = iota((1, 128), 1)
    q_of = div25(lane)
    b_of = lane - 25 * q_of
    pr = iota((160, 1), 0)
    pt, ps, pi = pr >> 5, (pr >> 3) & 3, pr & 7
    perm = onehot(jnp.where(pi < 6, 24 * pt + 4 * pi + ps, 9999) == iota((160, 128), 1))
    el = iota((128, 1), 0)
    expand = []
    for a in range(5):
        expand.append(onehot(jnp.where((b_of < 23) & (q_of < 5), 23 * a + b_of, 9999) == el))
    expand.append(onehot(jnp.broadcast_to(el == 120, (128, 128))))
    expand = jnp.concatenate(expand, axis=1)
    q_f = q_of.astype(F32)
    j_id = iota((32, 128), 0).astype(F32).astype(BF)

    ACC[...] = jnp.zeros_like(ACC)

    def consume(u):
        for p in range(4):
            px = jnp.dot(perm, LW[p, u], preferred_element_type=F32).astype(BF)
            for t in range(5):
                PX[t, pl.ds(32 * p, 32), :] = px[32 * t : 32 * t + 32]
        for t in range(5):
            width = 768 if t == 0 else 640
            ve = jnp.dot(PX[t], expand[:, :width], preferred_element_type=F32)
            for a in range(5):
                if 5 * t + a < 24:
                    VE[5 * t + a] = ve[:, 128 * a : 128 * a + 128]
            if t == 0:
                VE[24] = ve[:, 640:768] - q_f

        def left_tile(i, carry):
            p, m = i // 8, i % 8
            base = pl.multiple_of(p * 32, 32)
            col = pl.multiple_of(i * 128, 128)
            want = (5 * m).astype(F32)
            masks = [VE[24, pl.ds(base + 8 * s, 8), :] == want for s in range(4)]
            for ap in range(12):
                pair = []
                for a in (2 * ap, 2 * ap + 1):
                    v = jnp.zeros((8, 128), F32)
                    for s in range(4):
                        v = jnp.where(masks[s], VE[a, pl.ds(base + 8 * s, 8), :], v)
                    pair.append(v)
                LD[pl.ds(16 * ap, 16), pl.ds(col, 128)] = jnp.concatenate(pair, axis=0).astype(BF)
            return carry

        lax.fori_loop(0, 32, left_tile, 0)

        def right_tile(i, carry):
            p, m = i // 8, i % 8
            col = pl.multiple_of(i * 128, 128)
            block = RW[u, m % 2, m // 2, p]
            masks = [jnp.broadcast_to(block[24 * s + 23 : 24 * s + 24], (32, 128)) == j_id for s in range(3)]
            for c in range(23):
                v = jnp.zeros((32, 128), BF)
                for s in range(3):
                    v = jnp.where(masks[s], jnp.broadcast_to(block[24 * s + c : 24 * s + c + 1], (32, 128)), v)
                RT[pl.ds(32 * c, 32), pl.ds(col, 128)] = v
            return carry

        lax.fori_loop(0, 32, right_tile, 0)
        ACC[...] += lax.dot_general(RT[...], LD[...], (((1,), (1,)), ((), ())), preferred_element_type=F32)

    for o in range(1, 4):
        a_copy(o).wait_recv()
    own_right.wait()
    own_left.wait()
    z_copy(1).start()
    z_copy(2).start()

    def step(k, carry):
        @pl.when((k >= 1) & (k <= 6))
        def _():
            z_copy(k).wait_recv()

        @pl.when((k >= 1) & (k <= 4))
        def _():
            z_copy(k + 2).start()

        @pl.when((k == 5) | (k == 6))
        def _():
            zh_copy(k - 5).start()

        @pl.when(k == 7)
        def _():
            zh_copy(0).wait_recv()
            zh_copy(1).wait_recv()

        @pl.when(k <= 7)
        def _():
            x_copy(k, 0).start()
            x_copy(k, 1).start()

            @pl.when(k >= 1)
            def _():
                b_copy(k).wait_recv()

            y_copy(k, 0).start()
            y_copy(k, 1).start()

        @pl.when((k >= 1) & (k <= 8))
        def _():
            for h in range(2):
                x_copy(k - 1, h).wait_recv()
                xh_copy(k - 1, h).start()
            for h in range(2):
                y_copy(k - 1, h).wait_recv()
                yh_copy(k - 1, h).start()

        @pl.when((k >= 2) & (k <= 9))
        def _():
            for h in range(2):
                xh_copy(k - 2, h).wait_recv()
            d_copy(k - 2).start()
            for h in range(2):
                yh_copy(k - 2, h).wait_recv()

        @pl.when(k >= 3)
        def _():
            d_copy(k - 3).wait_recv()
            consume(unit(k - 3))

        return carry

    lax.fori_loop(0, 11, step, 0)

    mr = iota((144, 1), 0)
    mi = div23(mr)
    ma = mr - 23 * mi
    rows_pick = onehot(jnp.where(mr < 138, 8 * ma + mi, 9999) == iota((144, 192), 1))
    res = ACC[...].astype(BF)
    turned = lax.dot_general(rows_pick, res, (((1,), (1,)), ((), ())), preferred_element_type=F32).astype(BF)
    jj = div23(lane)
    cc = lane - 23 * jj
    ni = iota((736, 1), 0)
    for d in range(8):
        target = jnp.where(lane < 92, 32 * cc + 4 * d + jj, 9999)
        OS[d] = jnp.dot(turned, onehot(ni == target), preferred_element_type=F32).astype(BF)

    def o_copy(o):
        to = mod(z + o, 8)
        return copy(OS.at[to], out.at[z], o_s.at[o], o_r.at[o], (r, y, to))

    for o in range(1, 8):
        o_copy(o).start()
    own_out = pltpu.make_async_copy(OS.at[z], out.at[z], l_sem.at[2])
    own_out.start()

    for o in range(1, 4):
        a_copy(o).wait_send()

    def sent(k, carry):
        @pl.when(k >= 1)
        def _():
            b_copy(k).wait_send()

        @pl.when((k >= 1) & (k <= 6))
        def _():
            z_copy(k).wait_send()

        for h in range(2):
            x_copy(k, h).wait_send()
            xh_copy(k, h).wait_send()
            y_copy(k, h).wait_send()
            yh_copy(k, h).wait_send()
        d_copy(k).wait_send()
        return carry

    lax.fori_loop(0, 8, sent, 0)
    zh_copy(0).wait_send()
    zh_copy(1).wait_send()
    own_out.wait()
    for o in range(1, 8):
        o_copy(o).wait()


def body(left_values, left_columns, right_values, right_columns):
    left = jnp.concatenate([left_values, left_columns[..., None].astype(BF)], axis=3).reshape(192, SQ + 1)
    right = jnp.concatenate([right_values, right_columns[..., None].astype(BF)], axis=4).reshape(60, SQ + 1)
    vmem = pl.BlockSpec(memory_space=pltpu.VMEM)
    lws, rws = pl.pallas_call(
        prepare,
        out_shape=(jax.ShapeDtypeStruct((8, 128, 128), BF), jax.ShapeDtypeStruct((4, 72, 128), BF)),
        in_specs=[vmem, vmem],
        out_specs=(vmem, vmem),
        name="prepare",
    )(left, right)
    dma = pltpu.SemaphoreType.DMA
    pieces = pl.pallas_call(
        multiply,
        out_shape=jax.ShapeDtypeStruct((8, 144, 128), BF),
        in_specs=[vmem, vmem],
        out_specs=vmem,
        scratch_shapes=[
            pltpu.VMEM((4, 8, 128, 128), BF),
            pltpu.VMEM((8, 2, 4, 4, 72, 128), BF),
            pltpu.VMEM((5, 128, 128), BF),
            pltpu.VMEM((25, 128, 128), F32),
            pltpu.VMEM((192, 4096), BF),
            pltpu.VMEM((736, 4096), BF),
            pltpu.VMEM((736, 192), F32),
            pltpu.VMEM((8, 144, 128), BF),
            dma((3,)), dma((3,)),
            dma((8,)), dma((8,)),
            dma((9,)), dma((9,)),
            dma((2, 8)), dma((2, 8)),
            dma((2, 8)), dma((2, 8)),
            dma((2, 8)), dma((2, 8)),
            dma((2, 8)), dma((2, 8)),
            dma((8,)), dma((8,)),
            dma((8,)), dma((8,)),
            dma((3,)),
        ],
        compiler_params=pltpu.CompilerParams(collective_id=0, has_side_effects=True, vmem_limit_bytes=60 << 20),
        name="multiply",
    )(lws, rws)
    return pieces[:, :138, :92].reshape(1104, 92)


def solution(mesh):
    placed = (
        P("row", ("col", "depth"), None, None),
        P("row", ("col", "depth"), None),
        P(("col", "depth"), "row", None, None, None),
        P(("col", "depth"), "row", None, None),
    )
    return jax.shard_map(
        body, mesh=mesh, in_specs=placed, out_specs=P("row", ("col", "depth")), check_vma=False
    )
```

```python
import jax
import jax.numpy as jnp
from jax import lax
from jax.experimental import pallas as pl
from jax.experimental.pallas import tpu as pltpu
from jax.sharding import PartitionSpec as P

MESH = pl.DeviceIdType.MESH
BF = jnp.bfloat16
F32 = jnp.float32
I32 = jnp.int32
SQ = 529


def iota(shape, dim):
    return lax.broadcasted_iota(I32, shape, dim)


def onehot(cond):
    return jnp.where(cond, 1.0, 0.0).astype(BF)


def div25(lane):
    return (lane * 41) >> 10


def div23(n):
    return (n * 2850) >> 16


def fill_right(right, codes, rws):
    lane = iota((1, 128), 1)
    field = iota((SQ, 128), 0)
    row = iota((288, 1), 0)
    group = (row * 2731) >> 16
    c = row - 24 * group
    t = (group * 11) >> 5
    u = group - 3 * t
    f = iota((288, SQ), 1)
    keep = f - 23 * div23(f) == c
    q_of = div25(lane)
    b_of = lane - 25 * q_of
    total = jnp.zeros((288, 128), F32)
    for q in range(5):
        pick = onehot(iota((288, 60), 1) == 12 * q + 4 * u + t)
        spread = jnp.dot(pick, right, preferred_element_type=F32)
        spread = jnp.where(keep, spread, 0.0).astype(BF)
        low = jnp.where(q_of == q, 23 * b_of, 9999)
        total += jnp.dot(spread, onehot((field >= low) & (field < low + 23)), preferred_element_type=F32)
    q_hot = onehot(iota((5, 128), 0) == q_of)
    for v in range(3):
        wide = jnp.dot(codes[v].astype(F32).astype(BF), q_hot, preferred_element_type=F32).astype(BF)
        pick = onehot(iota((288, 4), 1) == jnp.where((u == v) & (c == 23), t, 9999))
        total += jnp.dot(pick, wide, preferred_element_type=F32)
    for k in range(4):
        rws[k] = total[72 * k : 72 * k + 72].astype(BF)


def fill_left(left, codes, lws):
    lane = iota((1, 128), 1)
    field = iota((SQ, 128), 0)
    row = iota((192, 1), 0)
    pick = onehot(iota((192, 48), 1) == row >> 2)
    codes = codes.astype(F32).astype(BF)
    code = lax.dot_general(pick, codes, (((1,), (1,)), ((), ())), preferred_element_type=F32)
    code = jnp.where(iota((192, 4), 1) == (row & 3), code, 0.0).astype(BF)
    tiles = []
    for t in range(5):
        target = jnp.where(lane < 115, 115 * t + lane, 9999)
        tile = jnp.dot(left, onehot(field == target), preferred_element_type=F32)
        if t == 0:
            place = onehot(jnp.broadcast_to(lane == 120, (4, 128)))
            tile += jnp.dot(code, place, preferred_element_type=F32)
        tiles.append(tile)
    for d in range(8):
        rows = [tile[24 * d : 24 * d + 24] for tile in tiles] + [jnp.zeros((8, 128), F32)]
        lws[d] = jnp.concatenate(rows, axis=0).astype(BF)


def multiply(
    left_ref, lcol_ref, right_ref, rcol_ref, out, lws, rws, LW, RW, LDA, LDB, ACC, OTHER, GS, OS,
    a_s, a_r, b_s, b_r, z_s, z_r, x_s, x_r, xh_s, xh_r, y_s, y_r, yh_s, yh_r, d_s, d_r, o_s, o_r, p_sem, l_sem,
):
    r, y, z = lax.axis_index("row"), lax.axis_index("col"), lax.axis_index("depth")
    x, e = r // 2, r % 2
    mod = lax.rem

    def zat(o):
        return (r, y, mod(z + o + 8, 8))

    def yat(o):
        return (r, mod(y + o + 4, 4), z)

    def xat(o):
        return (mod(r + 2 * o + 8, 8), y, z)

    partner = (r + 1 - 2 * e, y, z)
    friends = [zat(o) for o in range(1, 8)] + [yat(o) for o in range(1, 4)] + [xat(1), xat(-1), partner]
    barrier = pltpu.get_barrier_semaphore()
    for who in friends:
        pl.semaphore_signal(barrier, inc=1, device_id=who, device_id_type=MESH)
    fill_right(right_ref[...], rcol_ref, rws)

    def copy(src, dst, send, recv, who):
        return pltpu.make_async_remote_copy(
            src_ref=src, dst_ref=dst, send_sem=send, recv_sem=recv, device_id=who, device_id_type=MESH
        )

    def unit(k):
        odd = k % 2
        return mod(z + (1 - 2 * odd) * ((k + 1) // 2) + 8, 8)

    def a_copy(o):
        to = mod(y + o, 4)
        return copy(rws.at[to], RW.at[z, x, y], a_s.at[o - 1], a_r.at[o - 1], (r, to, z))

    def b_copy(k):
        odd = k % 2
        to = mod(z - (1 - 2 * odd) * ((k + 1) // 2) + 8, 8)
        return copy(lws.at[to], LW.at[e, y, z], b_s.at[k], b_r.at[k], (r, y, to))

    def z_copy(k):
        odd = k % 2
        step = 2 * odd - 1
        u = mod(z - (2 * odd - 1) * ((k + 1) // 2 - 1) + 8, 8)
        ref = RW.at[u, x]
        return copy(ref, ref, z_s.at[k], z_r.at[k], (r, y, mod(z + step + 8, 8)))

    def zh_copy(h):
        u = unit(5 + h)
        ref = RW.at[u, x, pl.ds(2 * h, 2)]
        return copy(ref, ref, z_s.at[7 + h], z_r.at[7 + h], zat(1 - 2 * h))

    def x_copy(k, h):
        ref = RW.at[unit(k), x]
        return copy(ref, ref, x_s.at[h, k], x_r.at[h, k], xat(1 - 2 * h))

    def xh_copy(k, h):
        ref = RW.at[unit(k), mod(x - (1 - 2 * h) + 4, 4), pl.ds(2 * h, 2)]
        return copy(ref, ref, xh_s.at[h, k], xh_r.at[h, k], xat(1 - 2 * h))

    def y_copy(k, h):
        ref = LW.at[e, y, unit(k)]
        return copy(ref, ref, y_s.at[h, k], y_r.at[h, k], yat(1 - 2 * h))

    def yh_copy(k, h):
        ref = LW.at[e, mod(y - (1 - 2 * h) + 4, 4), unit(k), pl.ds(64 * h, 64)]
        return copy(ref, ref, yh_s.at[h, k], yh_r.at[h, k], yat(1 - 2 * h))

    def d_copy(k):
        ref = LW.at[e, pl.ds(0, 4), unit(k)]
        return copy(ref, ref, d_s.at[k], d_r.at[k], partner)

    fill_left(left_ref[...], lcol_ref[...], lws)
    lane = iota((1, 128), 1)
    q_of = div25(lane)
    b_of = lane - 25 * q_of
    pr = iota((160, 1), 0)
    pt, ps, pi = pr >> 5, (pr >> 3) & 3, pr & 7
    perm = onehot(jnp.where(pi < 6, 24 * pt + 4 * pi + ps, 9999) == iota((160, 128), 1))
    el = iota((128, 1), 0)
    expand = []
    for a in range(5):
        expand.append(onehot(jnp.where((b_of < 23) & (q_of < 5), 23 * a + b_of, 9999) == el))
    expand.append(onehot(jnp.broadcast_to(el == 120, (128, 128))))
    expand = jnp.concatenate(expand, axis=1)
    q_f = (q_of + 5 * e).astype(F32)
    j_id = iota((32, 128), 0).astype(F32).astype(BF)

    ACC[...] = jnp.zeros_like(ACC)
    jj = div23(lane)
    cc = lane - 23 * jj
    ni = iota((736, 1), 0)
    for d in range(8):
        target = jnp.where(lane < 92, 32 * cc + 4 * d + jj, 9999)
        GS[:, pl.ds(128 * d, 128)] = onehot(ni == target)

    pl.semaphore_wait(barrier, len(friends))
    for o in range(1, 4):
        a_copy(o).start()
    own_right = pltpu.make_async_copy(rws.at[y], RW.at[z, x, y], l_sem.at[0])
    own_right.start()
    for k in range(1, 8):
        b_copy(k).start()
    own_left = pltpu.make_async_copy(lws.at[z], LW.at[e, y, z], l_sem.at[1])
    own_left.start()


    def fill(u, j, ld):
        px = []
        for st in range(2):
            for i in range(2):
                px.append(jnp.dot(perm, LW[st, 2 * j + i, u], preferred_element_type=F32).astype(BF))
        every = jnp.dot(jnp.concatenate(px, axis=0), expand, preferred_element_type=F32)
        for st in range(2):
            for i in range(2):
                ve = every[160 * (2 * st + i) : 160 * (2 * st + i) + 160]
                masks = []
                for s in range(4):
                    code = ve[8 * s : 8 * s + 8, 640:768] - q_f
                    code = jnp.concatenate([code, code], axis=0).astype(BF)
                    masks.append([code == jnp.array(10 * m, BF) for m in range(4)])
                for ap in range(12):
                    slots = []
                    for s in range(4):
                        pair = []
                        for a in (2 * ap, 2 * ap + 1):
                            t, w = a // 5, a % 5
                            pair.append(ve[32 * t + 8 * s : 32 * t + 8 * s + 8, 128 * w : 128 * w + 128])
                        slots.append(jnp.concatenate(pair, axis=0).astype(BF))
                    for m in range(4):
                        v = jnp.zeros((16, 128), BF)
                        for s in range(4):
                            v = jnp.where(masks[s][m], slots[s], v)
                        ld[st, pl.ds(16 * ap, 16), pl.ds(512 * i + 128 * m, 128)] = v

    def take(u, j, ld):
        tiles = []
        for m in range(8):
            block = RW[u, m % 4, 2 * j + m // 4]
            masks = [jnp.broadcast_to(block[24 * s + 23 : 24 * s + 24], (32, 128)) == j_id for s in range(3)]
            rows = []
            for c in range(23):
                v = jnp.zeros((32, 128), BF)
                for s in range(3):
                    v = jnp.where(masks[s], jnp.broadcast_to(block[24 * s + c : 24 * s + c + 1], (32, 128)), v)
                rows.append(v)
            tiles.append(jnp.concatenate(rows, axis=0))
        full = jnp.concatenate(tiles, axis=1)
        for st in range(2):
            ACC[st] += lax.dot_general(full, ld[st], (((1,), (1,)), ((), ())), preferred_element_type=F32)

    def x_start(k):
        x_copy(k, 0).start()
        x_copy(k, 1).start()

    def y_start(k):
        y_copy(k, 0).start()
        y_copy(k, 1).start()

    def x_forward(k):
        for h in range(2):
            x_copy(k, h).wait_recv()
            xh_copy(k, h).start()

    def y_forward(k):
        for h in range(2):
            y_copy(k, h).wait_recv()
            yh_copy(k, h).start()

    def x_done(k):
        for h in range(2):
            xh_copy(k, h).wait_recv()

    def y_done(k):
        for h in range(2):
            yh_copy(k, h).wait_recv()

    own_left.wait()
    y_start(0)
    for k in (1, 2):
        b_copy(k).wait_recv()
        y_start(k)
    for o in range(1, 4):
        a_copy(o).wait_recv()
    own_right.wait()
    z_copy(1).start()
    z_copy(2).start()
    x_start(0)
    y_forward(0)
    for k in (3, 4):
        b_copy(k).wait_recv()
        y_start(k)
    y_done(0)
    d_copy(0).start()
    for k in (1, 2):
        z_copy(k).wait_recv()
        z_copy(k + 2).start()
    x_start(1)
    x_forward(0)
    x_start(2)
    y_forward(1)
    y_forward(2)
    for k in (5, 6, 7):
        b_copy(k).wait_recv()
        y_start(k)
    d_copy(0).wait_recv()
    fill(unit(0), 0, LDA)
    x_forward(1)
    y_forward(3)
    y_forward(4)
    for k in (3, 4):
        z_copy(k).wait_recv()
        z_copy(k + 2).start()
    x_start(3)

    def step(k, carry):
        u = unit(k)

        @pl.when(k == 1)
        def _():
            for v in (5, 6):
                z_copy(v).wait_recv()
                zh_copy(v - 5).start()

        @pl.when(k <= 6)
        def _():
            y_done(k + 1)
            d_copy(k + 1).start()

        x_done(k)
        fill(u, 1, LDB)
        take(u, 0, LDA)

        @pl.when(k == 3)
        def _():
            zh_copy(0).wait_recv()
            zh_copy(1).wait_recv()

        @pl.when(k <= 5)
        def _():
            x_forward(k + 2)

        @pl.when(k <= 3)
        def _():
            x_start(k + 4)

        @pl.when(k == 0)
        def _():
            for v in (5, 6, 7):
                y_forward(v)

        @pl.when(k <= 6)
        def _():
            d_copy(k + 1).wait_recv()

        fill(unit(jnp.minimum(k + 1, 7)), 0, LDA)
        take(u, 1, LDB)
        return carry

    lax.fori_loop(0, 8, step, 0)
    p_copy = copy(ACC.at[1 - e], OTHER, p_sem.at[0], p_sem.at[1], partner)
    p_copy.start()
    p_copy.wait_recv()

    mr = iota((144, 1), 0)
    mi = div23(mr)
    ma = mr - 23 * mi
    rows_pick = onehot(jnp.where(mr < 138, 8 * ma + mi, 9999) == iota((144, 192), 1))
    res = (ACC[e] + OTHER[...]).astype(BF)
    turned = lax.dot_general(rows_pick, res, (((1,), (1,)), ((), ())), preferred_element_type=F32).astype(BF)
    spread = jnp.dot(turned, GS[...], preferred_element_type=F32).astype(BF)
    for d in range(8):
        OS[d] = spread[:, 128 * d : 128 * d + 128]

    def o_copy(o):
        to = mod(z + o, 8)
        return copy(OS.at[to], out.at[z], o_s.at[o], o_r.at[o], (r, y, to))

    for o in range(1, 8):
        o_copy(o).start()
    own_out = pltpu.make_async_copy(OS.at[z], out.at[z], l_sem.at[2])
    own_out.start()

    for o in range(1, 4):
        a_copy(o).wait_send()

    def sent(k, carry):
        @pl.when(k >= 1)
        def _():
            b_copy(k).wait_send()

        @pl.when((k >= 1) & (k <= 6))
        def _():
            z_copy(k).wait_send()

        for h in range(2):
            x_copy(k, h).wait_send()
            xh_copy(k, h).wait_send()
            y_copy(k, h).wait_send()
            yh_copy(k, h).wait_send()
        d_copy(k).wait_send()
        return carry

    lax.fori_loop(0, 8, sent, 0)
    zh_copy(0).wait_send()
    zh_copy(1).wait_send()
    own_out.wait()
    p_copy.wait_send()
    for o in range(1, 8):
        o_copy(o).wait()


def body(left_values, left_columns, right_values, right_columns):
    left = left_values.reshape(192, SQ)
    left_codes = jnp.transpose(left_columns[:, 0], (1, 0))
    right = jnp.transpose(right_values[0], (0, 2, 1, 3)).reshape(60, SQ)
    right_codes = jnp.transpose(right_columns[0], (2, 1, 0))
    vmem = pl.BlockSpec(memory_space=pltpu.VMEM)
    dma = pltpu.SemaphoreType.DMA
    pieces = pl.pallas_call(
        multiply,
        out_shape=jax.ShapeDtypeStruct((8, 144, 128), BF),
        in_specs=[vmem] * 4,
        out_specs=vmem,
        scratch_shapes=[
            pltpu.VMEM((8, 128, 128), BF),
            pltpu.VMEM((4, 72, 128), BF),
            pltpu.VMEM((2, 4, 8, 128, 128), BF),
            pltpu.VMEM((8, 4, 4, 72, 128), BF),
            pltpu.VMEM((2, 192, 1024), BF),
            pltpu.VMEM((2, 192, 1024), BF),
            pltpu.VMEM((2, 736, 192), F32),
            pltpu.VMEM((736, 192), F32),
            pltpu.VMEM((736, 1024), BF),
            pltpu.VMEM((8, 144, 128), BF),
            dma((3,)), dma((3,)),
            dma((8,)), dma((8,)),
            dma((9,)), dma((9,)),
            dma((2, 8)), dma((2, 8)),
            dma((2, 8)), dma((2, 8)),
            dma((2, 8)), dma((2, 8)),
            dma((2, 8)), dma((2, 8)),
            dma((8,)), dma((8,)),
            dma((8,)), dma((8,)),
            dma((2,)),
            dma((3,)),
        ],
        compiler_params=pltpu.CompilerParams(collective_id=0, has_side_effects=True, vmem_limit_bytes=24 << 20),
        name="multiply",
    )(left, left_codes, right, right_codes)
    return pieces[:, :138, :92].reshape(1104, 92)


def solution(mesh):
    placed = (
        P("row", ("col", "depth"), None, None),
        P("row", ("col", "depth"), None),
        P(("col", "depth"), "row", None, None, None),
        P(("col", "depth"), "row", None, None),
    )
    return jax.shard_map(
        body, mesh=mesh, in_specs=placed, out_specs=P("row", ("col", "depth")), check_vma=False
    )
```

```python
import jax
import jax.numpy as jnp
from jax import lax
from jax.experimental import pallas as pl
from jax.experimental.pallas import tpu as pltpu
from jax.sharding import PartitionSpec as P

MESH = pl.DeviceIdType.MESH
BF = jnp.bfloat16
F32 = jnp.float32
I32 = jnp.int32
SQ = 529


def iota(shape, dim):
    return lax.broadcasted_iota(I32, shape, dim)


def onehot(cond):
    return jnp.where(cond, 1.0, 0.0).astype(BF)


def div25(lane):
    return (lane * 41) >> 10


def div23(n):
    return (n * 2850) >> 16


def fill_right(right, codes, rws):
    lane = iota((1, 128), 1)
    field = iota((SQ, 128), 0)
    row = iota((288, 1), 0)
    group = (row * 2731) >> 16
    c = row - 24 * group
    t = (group * 11) >> 5
    u = group - 3 * t
    f = iota((288, SQ), 1)
    keep = f - 23 * div23(f) == c
    q_of = div25(lane)
    b_of = lane - 25 * q_of
    total = jnp.zeros((288, 128), F32)
    for q in range(5):
        pick = onehot(iota((288, 60), 1) == 12 * q + 4 * u + t)
        spread = jnp.dot(pick, right, preferred_element_type=F32)
        spread = jnp.where(keep, spread, 0.0).astype(BF)
        low = jnp.where(q_of == q, 23 * b_of, 9999)
        total += jnp.dot(spread, onehot((field >= low) & (field < low + 23)), preferred_element_type=F32)
    q_hot = onehot(iota((5, 128), 0) == q_of)
    for v in range(3):
        wide = jnp.dot(codes[v].astype(F32).astype(BF), q_hot, preferred_element_type=F32).astype(BF)
        pick = onehot(iota((288, 4), 1) == jnp.where((u == v) & (c == 23), t, 9999))
        total += jnp.dot(pick, wide, preferred_element_type=F32)
    for k in range(4):
        rws[k] = total[72 * k : 72 * k + 72].astype(BF)


def fill_left(left, codes, lws):
    lane = iota((1, 128), 1)
    field = iota((SQ, 128), 0)
    row = iota((256, 1), 0)
    s, i = (row >> 3) & 3, row & 7
    block_row = jnp.where(i < 6, 6 * (row >> 5) + i, 9999)
    picked = jnp.dot(onehot(iota((256, 192), 1) == 4 * block_row + s), left, preferred_element_type=F32).astype(BF)
    pick = onehot(iota((256, 48), 1) == block_row)
    codes = codes.astype(F32).astype(BF)
    code = lax.dot_general(pick, codes, (((1,), (1,)), ((), ())), preferred_element_type=F32)
    code = jnp.where(iota((256, 4), 1) == s, code, 0.0).astype(BF)
    for t in range(5):
        target = jnp.where(lane < 115, 115 * t + lane, 9999)
        tile = jnp.dot(picked, onehot(field == target), preferred_element_type=F32)
        if t == 0:
            place = onehot(jnp.broadcast_to(lane == 120, (4, 128)))
            tile += jnp.dot(code, place, preferred_element_type=F32)
        tile = tile.astype(BF)
        for d in range(8):
            lws[d, pl.ds(32 * t, 32), :] = tile[32 * d : 32 * d + 32]


def multiply(
    left_ref, lcol_ref, right_ref, rcol_ref, out, lws, rws, LW, RW, LDA, LDB, ACC, OTHER, GS, OS,
    a_s, a_r, b_s, b_r, z_s, z_r, x_s, x_r, xh_s, xh_r, y_s, y_r, yh_s, yh_r, d_s, d_r, o_s, o_r, p_sem, l_sem,
):
    r, y, z = lax.axis_index("row"), lax.axis_index("col"), lax.axis_index("depth")
    x, e = r // 2, r % 2
    mod = lax.rem

    def zat(o):
        return (r, y, mod(z + o + 8, 8))

    def yat(o):
        return (r, mod(y + o + 4, 4), z)

    def xat(o):
        return (mod(r + 2 * o + 8, 8), y, z)

    partner = (r + 1 - 2 * e, y, z)
    friends = [zat(o) for o in range(1, 8)] + [yat(o) for o in range(1, 4)] + [xat(1), xat(-1), partner]
    barrier = pltpu.get_barrier_semaphore()
    for who in friends:
        pl.semaphore_signal(barrier, inc=1, device_id=who, device_id_type=MESH)
    fill_right(right_ref[...], rcol_ref, rws)

    def copy(src, dst, send, recv, who):
        return pltpu.make_async_remote_copy(
            src_ref=src, dst_ref=dst, send_sem=send, recv_sem=recv, device_id=who, device_id_type=MESH
        )

    def unit(k):
        odd = k % 2
        return mod(z + (1 - 2 * odd) * ((k + 1) // 2) + 8, 8)

    def a_copy(o):
        to = mod(y + o, 4)
        return copy(rws.at[to], RW.at[z, x, y], a_s.at[o - 1], a_r.at[o - 1], (r, to, z))

    def b_copy(k):
        odd = k % 2
        to = mod(z - (1 - 2 * odd) * ((k + 1) // 2) + 8, 8)
        return copy(lws.at[to], LW.at[e, y, z], b_s.at[k], b_r.at[k], (r, y, to))

    def z_copy(k):
        odd = k % 2
        step = 2 * odd - 1
        u = mod(z - (2 * odd - 1) * ((k + 1) // 2 - 1) + 8, 8)
        ref = RW.at[u, x]
        return copy(ref, ref, z_s.at[k], z_r.at[k], (r, y, mod(z + step + 8, 8)))

    def zh_copy(h):
        u = unit(5 + h)
        ref = RW.at[u, x, pl.ds(2 * h, 2)]
        return copy(ref, ref, z_s.at[7 + h], z_r.at[7 + h], zat(1 - 2 * h))

    def x_copy(k, h):
        ref = RW.at[unit(k), x]
        return copy(ref, ref, x_s.at[h, k], x_r.at[h, k], xat(1 - 2 * h))

    def xh_copy(k, h):
        ref = RW.at[unit(k), mod(x - (1 - 2 * h) + 4, 4), pl.ds(2 * h, 2)]
        return copy(ref, ref, xh_s.at[h, k], xh_r.at[h, k], xat(1 - 2 * h))

    def y_copy(k, h):
        ref = LW.at[e, y, unit(k)]
        return copy(ref, ref, y_s.at[h, k], y_r.at[h, k], yat(1 - 2 * h))

    def y_first(h):
        return copy(lws.at[z], LW.at[e, y, z], y_s.at[h, 0], y_r.at[h, 0], yat(1 - 2 * h))

    def yh_copy(k, h):
        ref = LW.at[e, mod(y - (1 - 2 * h) + 4, 4), unit(k), pl.ds(80 * h, 80)]
        return copy(ref, ref, yh_s.at[h, k], yh_r.at[h, k], yat(1 - 2 * h))

    def d_copy(k):
        ref = LW.at[e, pl.ds(0, 4), unit(k)]
        return copy(ref, ref, d_s.at[k], d_r.at[k], partner)

    fill_left(left_ref[...], lcol_ref[...], lws)
    lane = iota((1, 128), 1)
    q_of = div25(lane)
    b_of = lane - 25 * q_of
    el = iota((128, 1), 0)
    expand = []
    for a in range(5):
        expand.append(onehot(jnp.where((b_of < 23) & (q_of < 5), 23 * a + b_of, 9999) == el))
    expand.append(onehot(jnp.broadcast_to(el == 120, (128, 128))))
    expand = jnp.concatenate(expand, axis=1)
    q_f = (q_of + 5 * e).astype(F32)
    j_id = iota((32, 128), 0).astype(F32).astype(BF)

    ACC[...] = jnp.zeros_like(ACC)
    jj = div23(lane)
    cc = lane - 23 * jj
    ni = iota((736, 1), 0)
    for d in range(8):
        target = jnp.where(lane < 92, 32 * cc + 4 * d + jj, 9999)
        GS[:, pl.ds(128 * d, 128)] = onehot(ni == target)

    pl.semaphore_wait(barrier, len(friends))
    for o in range(1, 4):
        a_copy(o).start()
    own_right = pltpu.make_async_copy(rws.at[y], RW.at[z, x, y], l_sem.at[0])
    own_right.start()
    own_left = pltpu.make_async_copy(lws.at[z], LW.at[e, y, z], l_sem.at[1])
    own_left.start()
    for h in range(2):
        y_first(h).start()
    for k in range(1, 8):
        b_copy(k).start()


    def fill(u, j, ld):
        px = []
        for st in range(2):
            for i in range(2):
                px.append(LW[st, 2 * j + i, u])
        every = jnp.dot(jnp.concatenate(px, axis=0), expand, preferred_element_type=F32)
        for st in range(2):
            for i in range(2):
                ve = every[160 * (2 * st + i) : 160 * (2 * st + i) + 160]
                masks = []
                for s in range(4):
                    code = ve[8 * s : 8 * s + 8, 640:768] - q_f
                    code = jnp.concatenate([code, code], axis=0).astype(BF)
                    masks.append([code == jnp.array(10 * m, BF) for m in range(4)])
                for ap in range(12):
                    slots = []
                    for s in range(4):
                        pair = []
                        for a in (2 * ap, 2 * ap + 1):
                            t, w = a // 5, a % 5
                            pair.append(ve[32 * t + 8 * s : 32 * t + 8 * s + 8, 128 * w : 128 * w + 128])
                        slots.append(jnp.concatenate(pair, axis=0).astype(BF))
                    for m in range(4):
                        v = jnp.zeros((16, 128), BF)
                        for s in range(4):
                            v = jnp.where(masks[s][m], slots[s], v)
                        ld[st, pl.ds(16 * ap, 16), pl.ds(512 * i + 128 * m, 128)] = v

    def take(u, j, ld):
        tiles = []
        for m in range(8):
            block = RW[u, m % 4, 2 * j + m // 4]
            masks = [jnp.broadcast_to(block[24 * s + 23 : 24 * s + 24], (32, 128)) == j_id for s in range(3)]
            rows = []
            for c in range(23):
                v = jnp.zeros((32, 128), BF)
                for s in range(3):
                    v = jnp.where(masks[s], jnp.broadcast_to(block[24 * s + c : 24 * s + c + 1], (32, 128)), v)
                rows.append(v)
            tiles.append(jnp.concatenate(rows, axis=0))
        full = jnp.concatenate(tiles, axis=1)
        for st in range(2):
            ACC[st] += lax.dot_general(full, ld[st], (((1,), (1,)), ((), ())), preferred_element_type=F32)

    def x_start(k):
        x_copy(k, 0).start()
        x_copy(k, 1).start()

    def y_start(k):
        y_copy(k, 0).start()
        y_copy(k, 1).start()

    def x_forward(k):
        for h in range(2):
            x_copy(k, h).wait_recv()
            xh_copy(k, h).start()

    def y_forward(k):
        for h in range(2):
            y_copy(k, h).wait_recv()
            yh_copy(k, h).start()

    def x_done(k):
        for h in range(2):
            xh_copy(k, h).wait_recv()

    def y_done(k):
        for h in range(2):
            yh_copy(k, h).wait_recv()

    for o in range(1, 4):
        a_copy(o).wait_recv()
    own_right.wait()
    z_copy(1).start()
    z_copy(2).start()
    x_start(0)
    y_forward(0)
    for k in (1, 2):
        b_copy(k).wait_recv()
        y_start(k)
    own_left.wait()
    y_done(0)
    d_copy(0).start()
    for k in (1, 2):
        z_copy(k).wait_recv()
        z_copy(k + 2).start()
    x_start(1)
    x_forward(0)
    x_start(2)
    for k in (3, 4):
        b_copy(k).wait_recv()
        y_start(k)
    d_copy(0).wait_recv()
    fill(unit(0), 0, LDA)
    y_forward(1)
    y_forward(2)
    for k in (5, 6, 7):
        b_copy(k).wait_recv()
        y_start(k)

    def step(k, carry):
        u = unit(k)

        @pl.when(k == 1)
        def _():
            x_forward(2)
            x_start(4)
            y_forward(5)
            y_forward(6)
            y_forward(7)

        @pl.when((k >= 1) & (k <= 6))
        def _():
            y_done(k + 1)
            d_copy(k + 1).start()

        x_done(k)
        fill(u, 1, LDB)
        take(u, 0, LDA)

        @pl.when(k == 0)
        def _():
            y_done(1)
            d_copy(1).start()
            x_forward(1)
            for v in (3, 4):
                z_copy(v).wait_recv()
                z_copy(v + 2).start()
            x_start(3)
            y_forward(3)
            y_forward(4)

        @pl.when(k == 1)
        def _():
            for v in (5, 6):
                z_copy(v).wait_recv()
                zh_copy(v - 5).start()

        @pl.when(k == 3)
        def _():
            zh_copy(0).wait_recv()
            zh_copy(1).wait_recv()

        @pl.when((k >= 1) & (k <= 5))
        def _():
            x_forward(k + 2)

        @pl.when((k >= 1) & (k <= 3))
        def _():
            x_start(k + 4)

        @pl.when(k <= 6)
        def _():
            d_copy(k + 1).wait_recv()

        fill(unit(jnp.minimum(k + 1, 7)), 0, LDA)
        take(u, 1, LDB)
        return carry

    lax.fori_loop(0, 8, step, 0)
    p_copy = copy(ACC.at[1 - e], OTHER, p_sem.at[0], p_sem.at[1], partner)
    p_copy.start()
    p_copy.wait_recv()

    mr = iota((144, 1), 0)
    mi = div23(mr)
    ma = mr - 23 * mi
    rows_pick = onehot(jnp.where(mr < 138, 8 * ma + mi, 9999) == iota((144, 192), 1))
    res = (ACC[e] + OTHER[...]).astype(BF)
    turned = lax.dot_general(rows_pick, res, (((1,), (1,)), ((), ())), preferred_element_type=F32).astype(BF)
    spread = jnp.dot(turned, GS[...], preferred_element_type=F32).astype(BF)
    for d in range(8):
        OS[d] = spread[:, 128 * d : 128 * d + 128]

    def o_copy(o):
        to = mod(z + o, 8)
        return copy(OS.at[to], out.at[z], o_s.at[o], o_r.at[o], (r, y, to))

    for o in (4, 3, 5, 2, 6, 1, 7):
        o_copy(o).start()
    own_out = pltpu.make_async_copy(OS.at[z], out.at[z], l_sem.at[2])
    own_out.start()

    for o in range(1, 4):
        a_copy(o).wait_send()

    def sent(k, carry):
        @pl.when(k >= 1)
        def _():
            b_copy(k).wait_send()

        @pl.when((k >= 1) & (k <= 6))
        def _():
            z_copy(k).wait_send()

        for h in range(2):
            x_copy(k, h).wait_send()
            xh_copy(k, h).wait_send()
            y_copy(k, h).wait_send()
            yh_copy(k, h).wait_send()
        d_copy(k).wait_send()
        return carry

    lax.fori_loop(0, 8, sent, 0)
    zh_copy(0).wait_send()
    zh_copy(1).wait_send()
    own_out.wait()
    p_copy.wait_send()
    for o in range(1, 8):
        o_copy(o).wait()


def body(left_values, left_columns, right_values, right_columns):
    left = left_values.reshape(192, SQ)
    left_codes = jnp.transpose(left_columns[:, 0], (1, 0))
    right = jnp.transpose(right_values[0], (0, 2, 1, 3)).reshape(60, SQ)
    right_codes = jnp.transpose(right_columns[0], (2, 1, 0))
    vmem = pl.BlockSpec(memory_space=pltpu.VMEM)
    dma = pltpu.SemaphoreType.DMA
    pieces = pl.pallas_call(
        multiply,
        out_shape=jax.ShapeDtypeStruct((8, 144, 128), BF),
        in_specs=[vmem] * 4,
        out_specs=vmem,
        scratch_shapes=[
            pltpu.VMEM((8, 160, 128), BF),
            pltpu.VMEM((4, 72, 128), BF),
            pltpu.VMEM((2, 4, 8, 160, 128), BF),
            pltpu.VMEM((8, 4, 4, 72, 128), BF),
            pltpu.VMEM((2, 192, 1024), BF),
            pltpu.VMEM((2, 192, 1024), BF),
            pltpu.VMEM((2, 736, 192), F32),
            pltpu.VMEM((736, 192), F32),
            pltpu.VMEM((736, 1024), BF),
            pltpu.VMEM((8, 144, 128), BF),
            dma((3,)), dma((3,)),
            dma((8,)), dma((8,)),
            dma((9,)), dma((9,)),
            dma((2, 8)), dma((2, 8)),
            dma((2, 8)), dma((2, 8)),
            dma((2, 8)), dma((2, 8)),
            dma((2, 8)), dma((2, 8)),
            dma((8,)), dma((8,)),
            dma((8,)), dma((8,)),
            dma((2,)),
            dma((3,)),
        ],
        compiler_params=pltpu.CompilerParams(collective_id=0, has_side_effects=True, vmem_limit_bytes=24 << 20),
        name="multiply",
    )(left, left_codes, right, right_codes)
    return pieces[:, :138, :92].reshape(1104, 92)


def solution(mesh):
    placed = (
        P("row", ("col", "depth"), None, None),
        P("row", ("col", "depth"), None),
        P(("col", "depth"), "row", None, None, None),
        P(("col", "depth"), "row", None, None),
    )
    return jax.shard_map(
        body, mesh=mesh, in_specs=placed, out_specs=P("row", ("col", "depth")), check_vma=False
    )
```

```python
import jax
import jax.numpy as jnp
from jax import lax
from jax.experimental import pallas as pl
from jax.experimental.pallas import tpu as pltpu
from jax.sharding import PartitionSpec as P

MESH = pl.DeviceIdType.MESH
BF = jnp.bfloat16
F32 = jnp.float32
I32 = jnp.int32
SQ = 529


def iota(shape, dim):
    return lax.broadcasted_iota(I32, shape, dim)


def onehot(cond):
    return jnp.where(cond, 1.0, 0.0).astype(BF)


def div25(lane):
    return (lane * 41) >> 10


def div23(n):
    return (n * 2850) >> 16


def fill_right(right, codes, rws):
    lane = iota((1, 128), 1)
    field = iota((SQ, 128), 0)
    row = iota((288, 1), 0)
    group = (row * 2731) >> 16
    c = row - 24 * group
    t = (group * 11) >> 5
    u = group - 3 * t
    f = iota((288, SQ), 1)
    keep = f - 23 * div23(f) == c
    q_of = div25(lane)
    b_of = lane - 25 * q_of
    total = jnp.zeros((288, 128), F32)
    for q in range(5):
        pick = onehot(iota((288, 60), 1) == 12 * q + 4 * u + t)
        spread = jnp.dot(pick, right, preferred_element_type=F32)
        spread = jnp.where(keep, spread, 0.0).astype(BF)
        low = jnp.where(q_of == q, 23 * b_of, 9999)
        total += jnp.dot(spread, onehot((field >= low) & (field < low + 23)), preferred_element_type=F32)
    q_hot = onehot(iota((5, 128), 0) == q_of)
    for v in range(3):
        wide = jnp.dot(codes[v].astype(F32).astype(BF), q_hot, preferred_element_type=F32).astype(BF)
        pick = onehot(iota((288, 4), 1) == jnp.where((u == v) & (c == 23), t, 9999))
        total += jnp.dot(pick, wide, preferred_element_type=F32)
    for k in range(4):
        rws[k] = total[72 * k : 72 * k + 72].astype(BF)


def fill_left(left, codes, lws):
    lane = iota((1, 128), 1)
    field = iota((SQ, 128), 0)
    row = iota((256, 1), 0)
    s, i = (row >> 3) & 3, row & 7
    block_row = jnp.where(i < 6, 6 * (row >> 5) + i, 9999)
    picked = jnp.dot(onehot(iota((256, 192), 1) == 4 * block_row + s), left, preferred_element_type=F32).astype(BF)
    pick = onehot(iota((256, 48), 1) == block_row)
    codes = codes.astype(F32).astype(BF)
    code = lax.dot_general(pick, codes, (((1,), (1,)), ((), ())), preferred_element_type=F32)
    code = jnp.where(iota((256, 4), 1) == s, code, 0.0).astype(BF)
    for t in range(5):
        target = jnp.where(lane < 115, 115 * t + lane, 9999)
        tile = jnp.dot(picked, onehot(field == target), preferred_element_type=F32)
        if t == 0:
            place = onehot(jnp.broadcast_to(lane == 120, (4, 128)))
            tile += jnp.dot(code, place, preferred_element_type=F32)
        tile = tile.astype(BF)
        for d in range(8):
            lws[d, pl.ds(32 * t, 32), :] = tile[32 * d : 32 * d + 32]


def multiply(
    left_ref, lcol_ref, right_ref, rcol_ref, out, lws, rws, LW, RW, LDA, LDB, ACC, OTHER, GS, OS,
    a_s, a_r, b_s, b_r, z_s, z_r, x_s, x_r, xh_s, xh_r, y_s, y_r, yh_s, yh_r, d_s, d_r, o_s, o_r, p_sem, l_sem,
):
    r, y, z = lax.axis_index("row"), lax.axis_index("col"), lax.axis_index("depth")
    x, e = r // 2, r % 2
    mod = lax.rem

    def zat(o):
        return (r, y, mod(z + o + 8, 8))

    def yat(o):
        return (r, mod(y + o + 4, 4), z)

    def xat(o):
        return (mod(r + 2 * o + 8, 8), y, z)

    partner = (r + 1 - 2 * e, y, z)
    friends = [zat(o) for o in range(1, 8)] + [yat(o) for o in range(1, 4)] + [xat(1), xat(-1), partner]
    barrier = pltpu.get_barrier_semaphore()
    for who in friends:
        pl.semaphore_signal(barrier, inc=1, device_id=who, device_id_type=MESH)
    fill_right(right_ref[...], rcol_ref, rws)

    def copy(src, dst, send, recv, who):
        return pltpu.make_async_remote_copy(
            src_ref=src, dst_ref=dst, send_sem=send, recv_sem=recv, device_id=who, device_id_type=MESH
        )

    def unit(k):
        odd = k % 2
        return mod(z + (1 - 2 * odd) * ((k + 1) // 2) + 8, 8)

    def a_copy(o):
        to = mod(y + o, 4)
        return copy(rws.at[to], RW.at[z, x, y], a_s.at[o - 1], a_r.at[o - 1], (r, to, z))

    def b_copy(k):
        odd = k % 2
        to = mod(z - (1 - 2 * odd) * ((k + 1) // 2) + 8, 8)
        return copy(lws.at[to], LW.at[e, y, z], b_s.at[k], b_r.at[k], (r, y, to))

    def z_copy(k):
        odd = k % 2
        step = 2 * odd - 1
        u = mod(z - (2 * odd - 1) * ((k + 1) // 2 - 1) + 8, 8)
        ref = RW.at[u, x]
        return copy(ref, ref, z_s.at[k], z_r.at[k], (r, y, mod(z + step + 8, 8)))

    def zh_copy(h):
        u = unit(5 + h)
        ref = RW.at[u, x, pl.ds(2 * h, 2)]
        return copy(ref, ref, z_s.at[7 + h], z_r.at[7 + h], zat(1 - 2 * h))

    def x_copy(k, h):
        ref = RW.at[unit(k), x]
        return copy(ref, ref, x_s.at[h, k], x_r.at[h, k], xat(1 - 2 * h))

    def xh_copy(k, h):
        ref = RW.at[unit(k), mod(x - (1 - 2 * h) + 4, 4), pl.ds(2 * h, 2)]
        return copy(ref, ref, xh_s.at[h, k], xh_r.at[h, k], xat(1 - 2 * h))

    def y_copy(k, h):
        ref = LW.at[e, y, unit(k)]
        return copy(ref, ref, y_s.at[h, k], y_r.at[h, k], yat(1 - 2 * h))

    def y_first(h):
        return copy(lws.at[z], LW.at[e, y, z], y_s.at[h, 0], y_r.at[h, 0], yat(1 - 2 * h))

    def yh_copy(k, h):
        ref = LW.at[e, mod(y - (1 - 2 * h) + 4, 4), unit(k), pl.ds(80 * h, 80)]
        return copy(ref, ref, yh_s.at[h, k], yh_r.at[h, k], yat(1 - 2 * h))

    def d_copy(k):
        ref = LW.at[e, pl.ds(0, 4), unit(k)]
        return copy(ref, ref, d_s.at[k], d_r.at[k], partner)

    fill_left(left_ref[...], lcol_ref[...], lws)
    lane = iota((1, 128), 1)
    q_of = div25(lane)
    b_of = lane - 25 * q_of
    el = iota((128, 1), 0)
    expand = []
    for a in range(5):
        expand.append(onehot(jnp.where((b_of < 23) & (q_of < 5), 23 * a + b_of, 9999) == el))
    expand.append(onehot(jnp.broadcast_to(el == 120, (128, 128))))
    expand = jnp.concatenate(expand, axis=1)
    q_f = (q_of + 5 * e).astype(F32)
    j_id = iota((32, 128), 0).astype(F32).astype(BF)

    ACC[...] = jnp.zeros_like(ACC)
    jj = div23(lane)
    cc = lane - 23 * jj
    ni = iota((736, 1), 0)
    for d in range(8):
        target = jnp.where(lane < 92, 32 * cc + 4 * d + jj, 9999)
        GS[:, pl.ds(128 * d, 128)] = onehot(ni == target)

    pl.semaphore_wait(barrier, len(friends))
    for o in range(1, 4):
        a_copy(o).start()
    own_right = pltpu.make_async_copy(rws.at[y], RW.at[z, x, y], l_sem.at[0])
    own_right.start()
    own_left = pltpu.make_async_copy(lws.at[z], LW.at[e, y, z], l_sem.at[1])
    own_left.start()
    for h in range(2):
        y_first(h).start()
    for k in (1, 2):
        b_copy(k).start()


    def fill(u, j, ld):
        px = []
        for st in range(2):
            for i in range(2):
                px.append(LW[st, 2 * j + i, u])
        every = jnp.dot(jnp.concatenate(px, axis=0), expand, preferred_element_type=F32)
        for st in range(2):
            for i in range(2):
                ve = every[160 * (2 * st + i) : 160 * (2 * st + i) + 160]
                masks = []
                for s in range(4):
                    code = ve[8 * s : 8 * s + 8, 640:768] - q_f
                    code = jnp.concatenate([code, code], axis=0).astype(BF)
                    masks.append([code == jnp.array(10 * m, BF) for m in range(4)])
                for ap in range(12):
                    slots = []
                    for s in range(4):
                        pair = []
                        for a in (2 * ap, 2 * ap + 1):
                            t, w = a // 5, a % 5
                            pair.append(ve[32 * t + 8 * s : 32 * t + 8 * s + 8, 128 * w : 128 * w + 128])
                        slots.append(jnp.concatenate(pair, axis=0).astype(BF))
                    for m in range(4):
                        v = jnp.zeros((16, 128), BF)
                        for s in range(4):
                            v = jnp.where(masks[s][m], slots[s], v)
                        ld[st, pl.ds(16 * ap, 16), pl.ds(512 * i + 128 * m, 128)] = v

    def take(u, j, ld):
        tiles = []
        for m in range(8):
            block = RW[u, m % 4, 2 * j + m // 4]
            masks = [jnp.broadcast_to(block[24 * s + 23 : 24 * s + 24], (32, 128)) == j_id for s in range(3)]
            rows = []
            for c in range(23):
                v = jnp.zeros((32, 128), BF)
                for s in range(3):
                    v = jnp.where(masks[s], jnp.broadcast_to(block[24 * s + c : 24 * s + c + 1], (32, 128)), v)
                rows.append(v)
            tiles.append(jnp.concatenate(rows, axis=0))
        full = jnp.concatenate(tiles, axis=1)
        for st in range(2):
            ACC[st] += lax.dot_general(full, ld[st], (((1,), (1,)), ((), ())), preferred_element_type=F32)

    def x_start(k):
        x_copy(k, 0).start()
        x_copy(k, 1).start()

    def y_start(k):
        y_copy(k, 0).start()
        y_copy(k, 1).start()

    def x_forward(k):
        for h in range(2):
            x_copy(k, h).wait_recv()
            xh_copy(k, h).start()

    def y_forward(k):
        for h in range(2):
            y_copy(k, h).wait_recv()
            yh_copy(k, h).start()

    def x_done(k):
        for h in range(2):
            xh_copy(k, h).wait_recv()

    def y_done(k):
        for h in range(2):
            yh_copy(k, h).wait_recv()

    for o in range(1, 4):
        a_copy(o).wait_recv()
    own_right.wait()
    z_copy(1).start()
    z_copy(2).start()
    x_start(0)
    y_forward(0)
    for k in range(3, 8):
        b_copy(k).start()
    for k in (1, 2):
        b_copy(k).wait_recv()
        y_start(k)
    own_left.wait()
    y_done(0)
    d_copy(0).start()
    x_forward(0)
    z_copy(1).wait_recv()
    z_copy(3).start()
    x_start(1)
    z_copy(2).wait_recv()
    z_copy(4).start()
    x_start(2)
    d_copy(0).wait_recv()
    fill(unit(0), 0, LDA)
    y_forward(1)
    y_forward(2)
    for k in (3, 4):
        b_copy(k).wait_recv()
        y_start(k)

    def step(k, carry):
        u = unit(k)

        @pl.when(k == 1)
        def _():
            x_forward(2)
            x_start(4)
            y_forward(5)
            y_forward(6)
            y_forward(7)

        @pl.when((k >= 1) & (k <= 6))
        def _():
            y_done(k + 1)
            d_copy(k + 1).start()

        x_done(k)
        fill(u, 1, LDB)
        take(u, 0, LDA)

        @pl.when(k == 0)
        def _():
            x_forward(1)
            y_done(1)
            d_copy(1).start()
            for v in (5, 6, 7):
                b_copy(v).wait_recv()
                y_start(v)
            for v in (3, 4):
                z_copy(v).wait_recv()
                z_copy(v + 2).start()
            x_start(3)
            y_forward(3)
            y_forward(4)

        @pl.when(k == 1)
        def _():
            for v in (5, 6):
                z_copy(v).wait_recv()
                zh_copy(v - 5).start()

        @pl.when(k == 3)
        def _():
            zh_copy(0).wait_recv()
            zh_copy(1).wait_recv()

        @pl.when((k >= 1) & (k <= 5))
        def _():
            x_forward(k + 2)

        @pl.when((k >= 1) & (k <= 3))
        def _():
            x_start(k + 4)

        @pl.when(k <= 6)
        def _():
            d_copy(k + 1).wait_recv()

        fill(unit(jnp.minimum(k + 1, 7)), 0, LDA)
        take(u, 1, LDB)
        return carry

    lax.fori_loop(0, 8, step, 0)
    p_copy = copy(ACC.at[1 - e], OTHER, p_sem.at[0], p_sem.at[1], partner)
    p_copy.start()
    p_copy.wait_recv()

    mr = iota((144, 1), 0)
    mi = div23(mr)
    ma = mr - 23 * mi
    rows_pick = onehot(jnp.where(mr < 138, 8 * ma + mi, 9999) == iota((144, 192), 1))
    res = (ACC[e] + OTHER[...]).astype(BF)
    turned = lax.dot_general(rows_pick, res, (((1,), (1,)), ((), ())), preferred_element_type=F32).astype(BF)
    spread = jnp.dot(turned, GS[...], preferred_element_type=F32).astype(BF)
    for d in range(8):
        OS[d] = spread[:, 128 * d : 128 * d + 128]

    def o_copy(o):
        to = mod(z + o, 8)
        return copy(OS.at[to], out.at[z], o_s.at[o], o_r.at[o], (r, y, to))

    for o in (4, 3, 5, 2, 6, 1, 7):
        o_copy(o).start()
    own_out = pltpu.make_async_copy(OS.at[z], out.at[z], l_sem.at[2])
    own_out.start()

    for o in range(1, 4):
        a_copy(o).wait_send()

    def sent(k, carry):
        @pl.when(k >= 1)
        def _():
            b_copy(k).wait_send()

        @pl.when((k >= 1) & (k <= 6))
        def _():
            z_copy(k).wait_send()

        for h in range(2):
            x_copy(k, h).wait_send()
            xh_copy(k, h).wait_send()
            y_copy(k, h).wait_send()
            yh_copy(k, h).wait_send()
        d_copy(k).wait_send()
        return carry

    lax.fori_loop(0, 8, sent, 0)
    zh_copy(0).wait_send()
    zh_copy(1).wait_send()
    own_out.wait()
    p_copy.wait_send()
    for o in range(1, 8):
        o_copy(o).wait()


def body(left_values, left_columns, right_values, right_columns):
    left = left_values.reshape(192, SQ)
    left_codes = jnp.transpose(left_columns[:, 0], (1, 0))
    right = jnp.transpose(right_values[0], (0, 2, 1, 3)).reshape(60, SQ)
    right_codes = jnp.transpose(right_columns[0], (2, 1, 0))
    vmem = pl.BlockSpec(memory_space=pltpu.VMEM)
    dma = pltpu.SemaphoreType.DMA
    pieces = pl.pallas_call(
        multiply,
        out_shape=jax.ShapeDtypeStruct((8, 144, 128), BF),
        in_specs=[vmem] * 4,
        out_specs=vmem,
        scratch_shapes=[
            pltpu.VMEM((8, 160, 128), BF),
            pltpu.VMEM((4, 72, 128), BF),
            pltpu.VMEM((2, 4, 8, 160, 128), BF),
            pltpu.VMEM((8, 4, 4, 72, 128), BF),
            pltpu.VMEM((2, 192, 1024), BF),
            pltpu.VMEM((2, 192, 1024), BF),
            pltpu.VMEM((2, 736, 192), F32),
            pltpu.VMEM((736, 192), F32),
            pltpu.VMEM((736, 1024), BF),
            pltpu.VMEM((8, 144, 128), BF),
            dma((3,)), dma((3,)),
            dma((8,)), dma((8,)),
            dma((9,)), dma((9,)),
            dma((2, 8)), dma((2, 8)),
            dma((2, 8)), dma((2, 8)),
            dma((2, 8)), dma((2, 8)),
            dma((2, 8)), dma((2, 8)),
            dma((8,)), dma((8,)),
            dma((8,)), dma((8,)),
            dma((2,)),
            dma((3,)),
        ],
        compiler_params=pltpu.CompilerParams(collective_id=0, has_side_effects=True, vmem_limit_bytes=24 << 20),
        name="multiply",
    )(left, left_codes, right, right_codes)
    return pieces[:, :138, :92].reshape(1104, 92)


def solution(mesh):
    placed = (
        P("row", ("col", "depth"), None, None),
        P("row", ("col", "depth"), None),
        P(("col", "depth"), "row", None, None, None),
        P(("col", "depth"), "row", None, None),
    )
    return jax.shard_map(
        body, mesh=mesh, in_specs=placed, out_specs=P("row", ("col", "depth")), check_vma=False
    )
```

```python
import jax
import jax.numpy as jnp
from jax import lax
from jax.experimental import pallas as pl
from jax.experimental.pallas import tpu as pltpu
from jax.sharding import PartitionSpec as P

MESH = pl.DeviceIdType.MESH
BF = jnp.bfloat16
F32 = jnp.float32
I32 = jnp.int32
SQ = 529


def iota(shape, dim):
    return lax.broadcasted_iota(I32, shape, dim)


def onehot(cond):
    return jnp.where(cond, 1.0, 0.0).astype(BF)


def div25(lane):
    return (lane * 41) >> 10


def div23(n):
    return (n * 2850) >> 16


def fill_right(right, codes, rws):
    lane = iota((1, 128), 1)
    field = iota((SQ, 128), 0)
    row = iota((288, 1), 0)
    group = (row * 2731) >> 16
    c = row - 24 * group
    t = (group * 11) >> 5
    u = group - 3 * t
    f = iota((288, SQ), 1)
    keep = f - 23 * div23(f) == c
    q_of = div25(lane)
    b_of = lane - 25 * q_of
    total = jnp.zeros((288, 128), F32)
    for q in range(5):
        pick = onehot(iota((288, 60), 1) == 12 * q + 4 * u + t)
        spread = jnp.dot(pick, right, preferred_element_type=F32)
        spread = jnp.where(keep, spread, 0.0).astype(BF)
        low = jnp.where(q_of == q, 23 * b_of, 9999)
        total += jnp.dot(spread, onehot((field >= low) & (field < low + 23)), preferred_element_type=F32)
    q_hot = onehot(iota((5, 128), 0) == q_of)
    for v in range(3):
        wide = jnp.dot(codes[v].astype(F32).astype(BF), q_hot, preferred_element_type=F32).astype(BF)
        pick = onehot(iota((288, 4), 1) == jnp.where((u == v) & (c == 23), t, 9999))
        total += jnp.dot(pick, wide, preferred_element_type=F32)
    for k in range(4):
        rws[k] = total[72 * k : 72 * k + 72].astype(BF)


def fill_left(left, codes, lws):
    lane = iota((1, 128), 1)
    field = iota((SQ, 128), 0)
    row = iota((256, 1), 0)
    s, i = (row >> 3) & 3, row & 7
    block_row = jnp.where(i < 6, 6 * (row >> 5) + i, 9999)
    picked = jnp.dot(onehot(iota((256, 192), 1) == 4 * block_row + s), left, preferred_element_type=F32).astype(BF)
    pick = onehot(iota((256, 48), 1) == block_row)
    codes = codes.astype(F32).astype(BF)
    code = lax.dot_general(pick, codes, (((1,), (1,)), ((), ())), preferred_element_type=F32)
    code = jnp.where(iota((256, 4), 1) == s, code, 0.0).astype(BF)
    for t in range(5):
        target = jnp.where(lane < 115, 115 * t + lane, 9999)
        tile = jnp.dot(picked, onehot(field == target), preferred_element_type=F32)
        if t == 0:
            place = onehot(jnp.broadcast_to(lane == 120, (4, 128)))
            tile += jnp.dot(code, place, preferred_element_type=F32)
        tile = tile.astype(BF)
        for d in range(8):
            lws[d, pl.ds(32 * t, 32), :] = tile[32 * d : 32 * d + 32]


def multiply(
    left_ref, lcol_ref, right_ref, rcol_ref, out, lws, rws, LW, RW, LDA, LDB, ACC, OTHER, GS, OS,
    a_s, a_r, b_s, b_r, z_s, z_r, x_s, x_r, xh_s, xh_r, y_s, y_r, yh_s, yh_r, d_s, d_r, o_s, o_r, p_sem, l_sem,
):
    r, y, z = lax.axis_index("row"), lax.axis_index("col"), lax.axis_index("depth")
    x, e = r // 2, r % 2
    mod = lax.rem

    def zat(o):
        return (r, y, mod(z + o + 8, 8))

    def yat(o):
        return (r, mod(y + o + 4, 4), z)

    def xat(o):
        return (mod(r + 2 * o + 8, 8), y, z)

    partner = (r + 1 - 2 * e, y, z)
    friends = [zat(o) for o in range(1, 8)] + [yat(o) for o in range(1, 4)] + [xat(1), xat(-1), partner]
    barrier = pltpu.get_barrier_semaphore()
    for who in friends:
        pl.semaphore_signal(barrier, inc=1, device_id=who, device_id_type=MESH)
    fill_right(right_ref[...], rcol_ref, rws)

    def copy(src, dst, send, recv, who):
        return pltpu.make_async_remote_copy(
            src_ref=src, dst_ref=dst, send_sem=send, recv_sem=recv, device_id=who, device_id_type=MESH
        )

    def unit(k):
        odd = k % 2
        return mod(z + (1 - 2 * odd) * ((k + 1) // 2) + 8, 8)

    def a_copy(o):
        to = mod(y + o, 4)
        return copy(rws.at[to], RW.at[z, x, y], a_s.at[o - 1], a_r.at[o - 1], (r, to, z))

    def b_copy(k):
        odd = k % 2
        to = mod(z - (1 - 2 * odd) * ((k + 1) // 2) + 8, 8)
        return copy(lws.at[to], LW.at[e, y, z], b_s.at[k], b_r.at[k], (r, y, to))

    def z_copy(k):
        odd = k % 2
        step = 2 * odd - 1
        u = mod(z - (2 * odd - 1) * ((k + 1) // 2 - 1) + 8, 8)
        ref = RW.at[u, x]
        return copy(ref, ref, z_s.at[k], z_r.at[k], (r, y, mod(z + step + 8, 8)))

    def zh_copy(h):
        u = unit(5 + h)
        ref = RW.at[u, x, pl.ds(2 * h, 2)]
        return copy(ref, ref, z_s.at[7 + h], z_r.at[7 + h], zat(1 - 2 * h))

    def x_copy(k, h):
        ref = RW.at[unit(k), x]
        return copy(ref, ref, x_s.at[h, k], x_r.at[h, k], xat(1 - 2 * h))

    def xh_copy(k, h):
        ref = RW.at[unit(k), mod(x - (1 - 2 * h) + 4, 4), pl.ds(2 * h, 2)]
        return copy(ref, ref, xh_s.at[h, k], xh_r.at[h, k], xat(1 - 2 * h))

    def y_copy(k, h):
        ref = LW.at[e, y, unit(k)]
        return copy(ref, ref, y_s.at[h, k], y_r.at[h, k], yat(1 - 2 * h))

    def y_first(h):
        return copy(lws.at[z], LW.at[e, y, z], y_s.at[h, 0], y_r.at[h, 0], yat(1 - 2 * h))

    def yh_copy(k, h):
        ref = LW.at[e, mod(y - (1 - 2 * h) + 4, 4), unit(k), pl.ds(80 * h, 80)]
        return copy(ref, ref, yh_s.at[h, k], yh_r.at[h, k], yat(1 - 2 * h))

    def d_copy(k):
        ref = LW.at[e, pl.ds(0, 4), unit(k)]
        return copy(ref, ref, d_s.at[k], d_r.at[k], partner)

    fill_left(left_ref[...], lcol_ref[...], lws)
    lane = iota((1, 128), 1)
    q_of = div25(lane)
    b_of = lane - 25 * q_of
    el = iota((128, 1), 0)
    expand = []
    for a in range(5):
        expand.append(onehot(jnp.where((b_of < 23) & (q_of < 5), 23 * a + b_of, 9999) == el))
    expand.append(onehot(jnp.broadcast_to(el == 120, (128, 128))))
    expand = jnp.concatenate(expand, axis=1)
    q_f = (q_of + 5 * e).astype(F32)
    j_id = iota((32, 128), 0).astype(F32).astype(BF)

    ACC[...] = jnp.zeros_like(ACC)
    for held in (LDA, LDB):
        for st in range(2):
            held[pl.ds(256 * st + 192, 64), :] = jnp.zeros((64, 1024), BF)
    jj = div23(lane)
    cc = lane - 23 * jj
    ni = iota((736, 1), 0)
    for d in range(8):
        target = jnp.where(lane < 92, 32 * cc + 4 * d + jj, 9999)
        GS[:, pl.ds(128 * d, 128)] = onehot(ni == target)

    pl.semaphore_wait(barrier, len(friends))
    for o in range(1, 4):
        a_copy(o).start()
    own_right = pltpu.make_async_copy(rws.at[y], RW.at[z, x, y], l_sem.at[0])
    own_right.start()
    own_left = pltpu.make_async_copy(lws.at[z], LW.at[e, y, z], l_sem.at[1])
    own_left.start()
    for h in range(2):
        y_first(h).start()
    for k in (1, 2):
        b_copy(k).start()


    def fill(u, j, ld):
        px = []
        for st in range(2):
            for i in range(2):
                px.append(LW[st, 2 * j + i, u])
        every = jnp.dot(jnp.concatenate(px, axis=0), expand, preferred_element_type=F32)
        for st in range(2):
            for i in range(2):
                ve = every[160 * (2 * st + i) : 160 * (2 * st + i) + 160]
                masks = []
                for s in range(4):
                    code = ve[8 * s : 8 * s + 8, 640:768] - q_f
                    code = jnp.concatenate([code, code], axis=0).astype(BF)
                    masks.append([code == jnp.array(10 * m, BF) for m in range(4)])
                for ap in range(12):
                    slots = []
                    for s in range(4):
                        pair = []
                        for a in (2 * ap, 2 * ap + 1):
                            t, w = a // 5, a % 5
                            pair.append(ve[32 * t + 8 * s : 32 * t + 8 * s + 8, 128 * w : 128 * w + 128])
                        slots.append(jnp.concatenate(pair, axis=0).astype(BF))
                    for m in range(4):
                        v = jnp.zeros((16, 128), BF)
                        for s in range(4):
                            v = jnp.where(masks[s][m], slots[s], v)
                        ld[pl.ds(256 * st + 16 * ap, 16), pl.ds(512 * i + 128 * m, 128)] = v

    def dense(u, j):
        tiles = []
        for m in range(8):
            block = RW[u, m % 4, 2 * j + m // 4]
            masks = [jnp.broadcast_to(block[24 * s + 23 : 24 * s + 24], (32, 128)) == j_id for s in range(3)]
            rows = []
            for c in range(23):
                v = jnp.zeros((32, 128), BF)
                for s in range(3):
                    v = jnp.where(masks[s], jnp.broadcast_to(block[24 * s + c : 24 * s + c + 1], (32, 128)), v)
                rows.append(v)
            tiles.append(jnp.concatenate(rows, axis=0))
        return jnp.concatenate(tiles, axis=1)

    def take(u, j, ld):
        ACC[...] += lax.dot_general(dense(u, j), ld[...], (((1,), (1,)), ((), ())), preferred_element_type=F32)

    def x_start(k):
        x_copy(k, 0).start()
        x_copy(k, 1).start()

    def y_start(k):
        y_copy(k, 0).start()
        y_copy(k, 1).start()

    def x_forward(k):
        for h in range(2):
            x_copy(k, h).wait_recv()
            xh_copy(k, h).start()

    def y_forward(k):
        for h in range(2):
            y_copy(k, h).wait_recv()
            yh_copy(k, h).start()

    def x_done(k):
        for h in range(2):
            xh_copy(k, h).wait_recv()

    def y_done(k):
        for h in range(2):
            yh_copy(k, h).wait_recv()

    for o in range(1, 4):
        a_copy(o).wait_recv()
    own_right.wait()
    z_copy(1).start()
    z_copy(2).start()
    x_start(0)
    y_forward(0)
    for k in range(3, 8):
        b_copy(k).start()
    for k in (1, 2):
        b_copy(k).wait_recv()
        y_start(k)
    own_left.wait()
    y_done(0)
    d_copy(0).start()
    x_forward(0)
    z_copy(1).wait_recv()
    z_copy(3).start()
    x_start(1)
    z_copy(2).wait_recv()
    z_copy(4).start()
    x_start(2)
    d_copy(0).wait_recv()
    fill(unit(0), 0, LDA)
    y_forward(1)
    y_forward(2)
    for k in (3, 4):
        b_copy(k).wait_recv()
        y_start(k)

    def step(k, carry):
        u = unit(k)

        @pl.when(k == 1)
        def _():
            x_forward(2)
            x_start(4)
            y_forward(5)
            y_forward(6)
            y_forward(7)

        @pl.when((k >= 1) & (k <= 6))
        def _():
            y_done(k + 1)
            d_copy(k + 1).start()

        x_done(k)
        fill(u, 1, LDB)
        take(u, 0, LDA)

        @pl.when(k == 0)
        def _():
            x_forward(1)
            y_done(1)
            d_copy(1).start()
            for v in (5, 6, 7):
                b_copy(v).wait_recv()
                y_start(v)
            for v in (3, 4):
                z_copy(v).wait_recv()
                z_copy(v + 2).start()
            x_start(3)
            y_forward(3)
            y_forward(4)

        @pl.when(k == 1)
        def _():
            for v in (5, 6):
                z_copy(v).wait_recv()
                zh_copy(v - 5).start()

        @pl.when(k == 3)
        def _():
            zh_copy(0).wait_recv()
            zh_copy(1).wait_recv()

        @pl.when((k >= 1) & (k <= 5))
        def _():
            x_forward(k + 2)

        @pl.when((k >= 1) & (k <= 3))
        def _():
            x_start(k + 4)

        @pl.when(k <= 6)
        def _():
            d_copy(k + 1).wait_recv()

        @pl.when(k <= 6)
        def _():
            fill(unit(k + 1), 0, LDA)
            take(u, 1, LDB)

        return carry

    lax.fori_loop(0, 8, step, 0)
    full = dense(unit(7), 1)
    theirs = pl.ds(pl.multiple_of(256 * (1 - e), 256), 256)
    ours = pl.ds(pl.multiple_of(256 * e, 256), 256)
    ACC[:, theirs] += lax.dot_general(full, LDB[theirs, :], (((1,), (1,)), ((), ())), preferred_element_type=F32)
    p_copy = copy(ACC.at[:, theirs], OTHER, p_sem.at[0], p_sem.at[1], partner)
    p_copy.start()
    ACC[:, ours] += lax.dot_general(full, LDB[ours, :], (((1,), (1,)), ((), ())), preferred_element_type=F32)
    p_copy.wait_recv()

    mr = iota((144, 1), 0)
    mi = div23(mr)
    ma = mr - 23 * mi
    rows_pick = onehot(jnp.where(mr < 138, 8 * ma + mi, 9999) == iota((144, 256), 1))
    res = (ACC[:, ours] + OTHER[...]).astype(BF)
    turned = lax.dot_general(rows_pick, res, (((1,), (1,)), ((), ())), preferred_element_type=F32).astype(BF)
    spread = jnp.dot(turned, GS[...], preferred_element_type=F32).astype(BF)
    for d in range(8):
        OS[d] = spread[:, 128 * d : 128 * d + 128]

    def o_copy(o):
        to = mod(z + o, 8)
        return copy(OS.at[to], out.at[z], o_s.at[o], o_r.at[o], (r, y, to))

    for o in (4, 3, 5, 2, 6, 1, 7):
        o_copy(o).start()
    own_out = pltpu.make_async_copy(OS.at[z], out.at[z], l_sem.at[2])
    own_out.start()

    for o in range(1, 4):
        a_copy(o).wait_send()

    def sent(k, carry):
        @pl.when(k >= 1)
        def _():
            b_copy(k).wait_send()

        @pl.when((k >= 1) & (k <= 6))
        def _():
            z_copy(k).wait_send()

        for h in range(2):
            x_copy(k, h).wait_send()
            xh_copy(k, h).wait_send()
            y_copy(k, h).wait_send()
            yh_copy(k, h).wait_send()
        d_copy(k).wait_send()
        return carry

    lax.fori_loop(0, 8, sent, 0)
    zh_copy(0).wait_send()
    zh_copy(1).wait_send()
    own_out.wait()
    p_copy.wait_send()
    for o in range(1, 8):
        o_copy(o).wait()


def body(left_values, left_columns, right_values, right_columns):
    left = left_values.reshape(192, SQ)
    left_codes = jnp.transpose(left_columns[:, 0], (1, 0))
    right = jnp.transpose(right_values[0], (0, 2, 1, 3)).reshape(60, SQ)
    right_codes = jnp.transpose(right_columns[0], (2, 1, 0))
    vmem = pl.BlockSpec(memory_space=pltpu.VMEM)
    dma = pltpu.SemaphoreType.DMA
    pieces = pl.pallas_call(
        multiply,
        out_shape=jax.ShapeDtypeStruct((8, 144, 128), BF),
        in_specs=[vmem] * 4,
        out_specs=vmem,
        scratch_shapes=[
            pltpu.VMEM((8, 160, 128), BF),
            pltpu.VMEM((4, 72, 128), BF),
            pltpu.VMEM((2, 4, 8, 160, 128), BF),
            pltpu.VMEM((8, 4, 4, 72, 128), BF),
            pltpu.VMEM((512, 1024), BF),
            pltpu.VMEM((512, 1024), BF),
            pltpu.VMEM((736, 512), F32),
            pltpu.VMEM((736, 256), F32),
            pltpu.VMEM((736, 1024), BF),
            pltpu.VMEM((8, 144, 128), BF),
            dma((3,)), dma((3,)),
            dma((8,)), dma((8,)),
            dma((9,)), dma((9,)),
            dma((2, 8)), dma((2, 8)),
            dma((2, 8)), dma((2, 8)),
            dma((2, 8)), dma((2, 8)),
            dma((2, 8)), dma((2, 8)),
            dma((8,)), dma((8,)),
            dma((8,)), dma((8,)),
            dma((2,)),
            dma((3,)),
        ],
        compiler_params=pltpu.CompilerParams(collective_id=0, has_side_effects=True, vmem_limit_bytes=24 << 20),
        name="multiply",
    )(left, left_codes, right, right_codes)
    return pieces[:, :138, :92].reshape(1104, 92)


def solution(mesh):
    placed = (
        P("row", ("col", "depth"), None, None),
        P("row", ("col", "depth"), None),
        P(("col", "depth"), "row", None, None, None),
        P(("col", "depth"), "row", None, None),
    )
    return jax.shard_map(
        body, mesh=mesh, in_specs=placed, out_specs=P("row", ("col", "depth")), check_vma=False
    )
```

```python
import jax
import jax.numpy as jnp
from jax import lax
from jax.experimental import pallas as pl
from jax.experimental.pallas import tpu as pltpu
from jax.sharding import PartitionSpec as P

MESH = pl.DeviceIdType.MESH
BF = jnp.bfloat16
F32 = jnp.float32
I32 = jnp.int32
SQ = 529


def iota(shape, dim):
    return lax.broadcasted_iota(I32, shape, dim)


def onehot(cond):
    return jnp.where(cond, 1.0, 0.0).astype(BF)


def div25(lane):
    return (lane * 41) >> 10


def div23(n):
    return (n * 2850) >> 16


def fill_right(right, codes, rws):
    lane = iota((1, 128), 1)
    field = iota((SQ, 128), 0)
    row = iota((288, 1), 0)
    group = (row * 2731) >> 16
    c = row - 24 * group
    t = (group * 11) >> 5
    u = group - 3 * t
    f = iota((288, SQ), 1)
    keep = f - 23 * div23(f) == c
    q_of = div25(lane)
    b_of = lane - 25 * q_of
    total = jnp.zeros((288, 128), F32)
    for q in range(5):
        pick = onehot(iota((288, 60), 1) == 12 * q + 4 * u + t)
        spread = jnp.dot(pick, right, preferred_element_type=F32)
        spread = jnp.where(keep, spread, 0.0).astype(BF)
        low = jnp.where(q_of == q, 23 * b_of, 9999)
        total += jnp.dot(spread, onehot((field >= low) & (field < low + 23)), preferred_element_type=F32)
    q_hot = onehot(iota((5, 128), 0) == q_of)
    for v in range(3):
        wide = jnp.dot(codes[v].astype(F32).astype(BF), q_hot, preferred_element_type=F32).astype(BF)
        pick = onehot(iota((288, 4), 1) == jnp.where((u == v) & (c == 23), t, 9999))
        total += jnp.dot(pick, wide, preferred_element_type=F32)
    for k in range(4):
        rws[k] = total[72 * k : 72 * k + 72].astype(BF)


def fill_left(left, codes, lws):
    lane = iota((1, 128), 1)
    field = iota((SQ, 128), 0)
    row = iota((256, 1), 0)
    s, i = (row >> 3) & 3, row & 7
    block_row = jnp.where(i < 6, 6 * (row >> 5) + i, 9999)
    picked = jnp.dot(onehot(iota((256, 192), 1) == 4 * block_row + s), left, preferred_element_type=F32).astype(BF)
    pick = onehot(iota((256, 48), 1) == block_row)
    codes = codes.astype(F32).astype(BF)
    code = lax.dot_general(pick, codes, (((1,), (1,)), ((), ())), preferred_element_type=F32)
    code = jnp.where(iota((256, 4), 1) == s, code, 0.0).astype(BF)
    for t in range(5):
        target = jnp.where(lane < 115, 115 * t + lane, 9999)
        tile = jnp.dot(picked, onehot(field == target), preferred_element_type=F32)
        if t == 0:
            place = onehot(jnp.broadcast_to(lane == 120, (4, 128)))
            tile += jnp.dot(code, place, preferred_element_type=F32)
        tile = tile.astype(BF)
        for d in range(8):
            lws[d, pl.ds(32 * t, 32), :] = tile[32 * d : 32 * d + 32]


def multiply(
    left_ref, lcol_ref, right_ref, rcol_ref, out, lws, rws, LW, RW, LDA, LDB, ACC, OTHER, GS, OS,
    a_s, a_r, b_s, b_r, z_s, z_r, x_s, x_r, xh_s, xh_r, y_s, y_r, yh_s, yh_r, d_s, d_r, o_s, o_r, p_sem, l_sem,
):
    r, y, z = lax.axis_index("row"), lax.axis_index("col"), lax.axis_index("depth")
    x, e = r // 2, r % 2
    mod = lax.rem

    def zat(o):
        return (r, y, mod(z + o + 8, 8))

    def yat(o):
        return (r, mod(y + o + 4, 4), z)

    def xat(o):
        return (mod(r + 2 * o + 8, 8), y, z)

    partner = (r + 1 - 2 * e, y, z)
    friends = [zat(o) for o in range(1, 8)] + [yat(o) for o in range(1, 4)] + [xat(1), xat(-1), partner]
    barrier = pltpu.get_barrier_semaphore()
    for who in friends:
        pl.semaphore_signal(barrier, inc=1, device_id=who, device_id_type=MESH)
    fill_right(right_ref[...], rcol_ref, rws)

    def copy(src, dst, send, recv, who):
        return pltpu.make_async_remote_copy(
            src_ref=src, dst_ref=dst, send_sem=send, recv_sem=recv, device_id=who, device_id_type=MESH
        )

    def unit(k):
        odd = k % 2
        return mod(z + (1 - 2 * odd) * ((k + 1) // 2) + 8, 8)

    def a_copy(o):
        to = mod(y + o, 4)
        return copy(rws.at[to], RW.at[z, x, y], a_s.at[o - 1], a_r.at[o - 1], (r, to, z))

    def b_copy(k):
        odd = k % 2
        to = mod(z - (1 - 2 * odd) * ((k + 1) // 2) + 8, 8)
        return copy(lws.at[to], LW.at[e, y, z], b_s.at[k], b_r.at[k], (r, y, to))

    def z_copy(k):
        odd = k % 2
        step = 2 * odd - 1
        u = mod(z - (2 * odd - 1) * ((k + 1) // 2 - 1) + 8, 8)
        ref = RW.at[u, x]
        return copy(ref, ref, z_s.at[k], z_r.at[k], (r, y, mod(z + step + 8, 8)))

    def zh_copy(h):
        u = unit(5 + h)
        ref = RW.at[u, x, pl.ds(2 * h, 2)]
        return copy(ref, ref, z_s.at[7 + h], z_r.at[7 + h], zat(1 - 2 * h))

    def x_copy(k, h):
        ref = RW.at[unit(k), x]
        return copy(ref, ref, x_s.at[h, k], x_r.at[h, k], xat(1 - 2 * h))

    def xh_copy(k, h):
        ref = RW.at[unit(k), mod(x - (1 - 2 * h) + 4, 4), pl.ds(2 * h, 2)]
        return copy(ref, ref, xh_s.at[h, k], xh_r.at[h, k], xat(1 - 2 * h))

    def y_copy(k, h):
        ref = LW.at[e, y, unit(k)]
        return copy(ref, ref, y_s.at[h, k], y_r.at[h, k], yat(1 - 2 * h))

    def y_first(h):
        return copy(lws.at[z], LW.at[e, y, z], y_s.at[h, 0], y_r.at[h, 0], yat(1 - 2 * h))

    def yh_copy(k, h):
        ref = LW.at[e, mod(y - (1 - 2 * h) + 4, 4), unit(k), pl.ds(80 * h, 80)]
        return copy(ref, ref, yh_s.at[h, k], yh_r.at[h, k], yat(1 - 2 * h))

    def d_copy(k):
        ref = LW.at[e, pl.ds(0, 4), unit(k)]
        return copy(ref, ref, d_s.at[k], d_r.at[k], partner)

    fill_left(left_ref[...], lcol_ref[...], lws)
    lane = iota((1, 128), 1)
    q_of = div25(lane)
    b_of = lane - 25 * q_of
    el = iota((128, 1), 0)
    expand = []
    for a in range(5):
        expand.append(onehot(jnp.where((b_of < 23) & (q_of < 5), 23 * a + b_of, 9999) == el))
    expand.append(onehot(jnp.broadcast_to(el == 120, (128, 128))))
    expand = jnp.concatenate(expand, axis=1)
    q_f = (q_of + 5 * e).astype(F32)
    j_id = iota((32, 128), 0).astype(F32).astype(BF)

    ACC[...] = jnp.zeros_like(ACC)
    for held in (LDA, LDB):
        for st in range(2):
            held[pl.ds(256 * st + 192, 64), :] = jnp.zeros((64, 1024), BF)
    jj = div23(lane)
    cc = lane - 23 * jj
    ni = iota((736, 1), 0)
    for d in range(8):
        target = jnp.where(lane < 92, 32 * cc + 4 * d + jj, 9999)
        GS[:, pl.ds(128 * d, 128)] = onehot(ni == target)

    pl.semaphore_wait(barrier, len(friends))
    for o in range(1, 4):
        a_copy(o).start()
    own_right = pltpu.make_async_copy(rws.at[y], RW.at[z, x, y], l_sem.at[0])
    own_right.start()
    own_left = pltpu.make_async_copy(lws.at[z], LW.at[e, y, z], l_sem.at[1])
    own_left.start()
    for h in range(2):
        y_first(h).start()
    for k in (1, 2):
        b_copy(k).start()


    def fill(u, j, ld):
        px = []
        for st in range(2):
            for i in range(2):
                px.append(LW[st, 2 * j + i, u])
        every = jnp.dot(jnp.concatenate(px, axis=0), expand, preferred_element_type=F32)
        for st in range(2):
            for i in range(2):
                ve = every[160 * (2 * st + i) : 160 * (2 * st + i) + 160]
                masks = []
                for s in range(4):
                    code = ve[8 * s : 8 * s + 8, 640:768] - q_f
                    code = jnp.concatenate([code, code], axis=0).astype(BF)
                    masks.append([code == jnp.array(10 * m, BF) for m in range(4)])
                for ap in range(12):
                    slots = []
                    for s in range(4):
                        pair = []
                        for a in (2 * ap, 2 * ap + 1):
                            t, w = a // 5, a % 5
                            pair.append(ve[32 * t + 8 * s : 32 * t + 8 * s + 8, 128 * w : 128 * w + 128])
                        slots.append(jnp.concatenate(pair, axis=0).astype(BF))
                    for m in range(4):
                        v = jnp.zeros((16, 128), BF)
                        for s in range(4):
                            v = jnp.where(masks[s][m], slots[s], v)
                        ld[pl.ds(256 * st + 16 * ap, 16), pl.ds(512 * i + 128 * m, 128)] = v

    def dense(u, j):
        tiles = []
        for m in range(8):
            block = RW[u, m % 4, 2 * j + m // 4]
            masks = [jnp.broadcast_to(block[24 * s + 23 : 24 * s + 24], (32, 128)) == j_id for s in range(3)]
            rows = []
            for c in range(23):
                v = jnp.zeros((32, 128), BF)
                for s in range(3):
                    v = jnp.where(masks[s], jnp.broadcast_to(block[24 * s + c : 24 * s + c + 1], (32, 128)), v)
                rows.append(v)
            tiles.append(jnp.concatenate(rows, axis=0))
        return jnp.concatenate(tiles, axis=1)

    def take(u, j, ld):
        ACC[...] += lax.dot_general(dense(u, j), ld[...], (((1,), (1,)), ((), ())), preferred_element_type=F32)

    def x_start(k):
        x_copy(k, 0).start()
        x_copy(k, 1).start()

    def y_start(k):
        y_copy(k, 0).start()
        y_copy(k, 1).start()

    def x_forward(k):
        for h in range(2):
            x_copy(k, h).wait_recv()
            xh_copy(k, h).start()

    def y_forward(k):
        for h in range(2):
            y_copy(k, h).wait_recv()
            yh_copy(k, h).start()

    def x_done(k):
        for h in range(2):
            xh_copy(k, h).wait_recv()

    def y_done(k):
        for h in range(2):
            yh_copy(k, h).wait_recv()

    for o in range(1, 4):
        a_copy(o).wait_recv()
    own_right.wait()
    z_copy(1).start()
    z_copy(2).start()
    x_start(0)
    y_forward(0)
    for k in range(3, 8):
        b_copy(k).start()
    for k in (1, 2):
        b_copy(k).wait_recv()
        y_start(k)
    own_left.wait()
    y_done(0)
    d_copy(0).start()
    x_forward(0)
    z_copy(1).wait_recv()
    z_copy(3).start()
    x_start(1)
    z_copy(2).wait_recv()
    z_copy(4).start()
    x_start(2)
    d_copy(0).wait_recv()
    fill(unit(0), 0, LDA)
    y_forward(1)
    y_forward(2)
    for k in (3, 4):
        b_copy(k).wait_recv()
        y_start(k)

    def step(k, carry):
        u = unit(k)

        @pl.when(k == 1)
        def _():
            x_forward(2)
            x_start(4)
            y_forward(5)
            y_forward(6)
            y_forward(7)

        @pl.when((k >= 1) & (k <= 6))
        def _():
            y_done(k + 1)
            d_copy(k + 1).start()

        x_done(k)
        fill(u, 1, LDB)
        take(u, 0, LDA)

        @pl.when(k == 0)
        def _():
            x_forward(1)
            y_done(1)
            d_copy(1).start()
            for v in (5, 6, 7):
                b_copy(v).wait_recv()
                y_start(v)
            for v in (3, 4):
                z_copy(v).wait_recv()
                z_copy(v + 2).start()
            x_start(3)
            y_forward(3)
            y_forward(4)

        @pl.when(k == 1)
        def _():
            for v in (5, 6):
                z_copy(v).wait_recv()
                zh_copy(v - 5).start()

        @pl.when(k == 3)
        def _():
            zh_copy(0).wait_recv()
            zh_copy(1).wait_recv()

        @pl.when((k >= 1) & (k <= 2))
        def _():
            x_forward(k + 2)

        @pl.when((k >= 1) & (k <= 3))
        def _():
            x_start(k + 4)

        @pl.when((k >= 2) & (k <= 4))
        def _():
            x_forward(k + 3)

        @pl.when(k <= 6)
        def _():
            d_copy(k + 1).wait_recv()

        @pl.when(k <= 6)
        def _():
            fill(unit(k + 1), 0, LDA)
            take(u, 1, LDB)

        return carry

    lax.fori_loop(0, 8, step, 0)
    full = dense(unit(7), 1)
    theirs = pl.ds(pl.multiple_of(256 * (1 - e), 256), 256)
    ours = pl.ds(pl.multiple_of(256 * e, 256), 256)
    ACC[:, theirs] += lax.dot_general(full, LDB[theirs, :], (((1,), (1,)), ((), ())), preferred_element_type=F32)
    p_copy = copy(ACC.at[:, theirs], OTHER, p_sem.at[0], p_sem.at[1], partner)
    p_copy.start()
    ACC[:, ours] += lax.dot_general(full, LDB[ours, :], (((1,), (1,)), ((), ())), preferred_element_type=F32)
    p_copy.wait_recv()

    mr = iota((144, 1), 0)
    mi = div23(mr)
    ma = mr - 23 * mi
    rows_pick = onehot(jnp.where(mr < 138, 8 * ma + mi, 9999) == iota((144, 256), 1))
    res = (ACC[:, ours] + OTHER[...]).astype(BF)
    turned = lax.dot_general(rows_pick, res, (((1,), (1,)), ((), ())), preferred_element_type=F32).astype(BF)
    spread = jnp.dot(turned, GS[...], preferred_element_type=F32).astype(BF)
    for d in range(8):
        OS[d] = spread[:, 128 * d : 128 * d + 128]

    def o_copy(o):
        to = mod(z + o, 8)
        return copy(OS.at[to], out.at[z], o_s.at[o], o_r.at[o], (r, y, to))

    for o in (4, 3, 5, 2, 6, 1, 7):
        o_copy(o).start()
    own_out = pltpu.make_async_copy(OS.at[z], out.at[z], l_sem.at[2])
    own_out.start()

    for o in range(1, 4):
        a_copy(o).wait_send()

    def sent(k, carry):
        @pl.when(k >= 1)
        def _():
            b_copy(k).wait_send()

        @pl.when((k >= 1) & (k <= 6))
        def _():
            z_copy(k).wait_send()

        for h in range(2):
            x_copy(k, h).wait_send()
            xh_copy(k, h).wait_send()
            y_copy(k, h).wait_send()
            yh_copy(k, h).wait_send()
        d_copy(k).wait_send()
        return carry

    lax.fori_loop(0, 8, sent, 0)
    zh_copy(0).wait_send()
    zh_copy(1).wait_send()
    own_out.wait()
    p_copy.wait_send()
    for o in range(1, 8):
        o_copy(o).wait()


def body(left_values, left_columns, right_values, right_columns):
    left = left_values.reshape(192, SQ)
    left_codes = jnp.transpose(left_columns[:, 0], (1, 0))
    right = jnp.transpose(right_values[0], (0, 2, 1, 3)).reshape(60, SQ)
    right_codes = jnp.transpose(right_columns[0], (2, 1, 0))
    vmem = pl.BlockSpec(memory_space=pltpu.VMEM)
    dma = pltpu.SemaphoreType.DMA
    pieces = pl.pallas_call(
        multiply,
        out_shape=jax.ShapeDtypeStruct((8, 144, 128), BF),
        in_specs=[vmem] * 4,
        out_specs=vmem,
        scratch_shapes=[
            pltpu.VMEM((8, 160, 128), BF),
            pltpu.VMEM((4, 72, 128), BF),
            pltpu.VMEM((2, 4, 8, 160, 128), BF),
            pltpu.VMEM((8, 4, 4, 72, 128), BF),
            pltpu.VMEM((512, 1024), BF),
            pltpu.VMEM((512, 1024), BF),
            pltpu.VMEM((736, 512), F32),
            pltpu.VMEM((736, 256), F32),
            pltpu.VMEM((736, 1024), BF),
            pltpu.VMEM((8, 144, 128), BF),
            dma((3,)), dma((3,)),
            dma((8,)), dma((8,)),
            dma((9,)), dma((9,)),
            dma((2, 8)), dma((2, 8)),
            dma((2, 8)), dma((2, 8)),
            dma((2, 8)), dma((2, 8)),
            dma((2, 8)), dma((2, 8)),
            dma((8,)), dma((8,)),
            dma((8,)), dma((8,)),
            dma((2,)),
            dma((3,)),
        ],
        compiler_params=pltpu.CompilerParams(collective_id=0, has_side_effects=True, vmem_limit_bytes=24 << 20),
        name="multiply",
    )(left, left_codes, right, right_codes)
    return pieces[:, :138, :92].reshape(1104, 92)


def solution(mesh):
    placed = (
        P("row", ("col", "depth"), None, None),
        P("row", ("col", "depth"), None),
        P(("col", "depth"), "row", None, None, None),
        P(("col", "depth"), "row", None, None),
    )
    return jax.shard_map(
        body, mesh=mesh, in_specs=placed, out_specs=P("row", ("col", "depth")), check_vma=False
    )
```
